768 devices in a mesh: dp: 4 (over y_lo, core), expert: 48 (over z, y_hi), tensor: 4 (over x).
Axes of the slice: x: 4, y: 8 (y_hi: 4, y_lo: 2; y = y_hi * 2 + y_lo), z: 12, core: 2. Of those that a mesh axis runs over, the one named last changes fastest.
Arguments:
- tokens: bfloat16 [3072, 3072], P(('dp', 'expert')), may hold values from -45 to 45
- cotangent: bfloat16 [3072, 3072], P(('dp', 'expert')), may hold values from -6 to 6
- gain: float32 [3072], replicated, may hold values from 0.5 to 1.5
- w_router: bfloat16 [3072, 8], replicated, may hold values from -0.109375 to 0.109375
- w_gate: bfloat16 [48, 3072, 1536], P('expert', None, 'tensor'), may hold values from -0.109375 to 0.109375
- w_up: bfloat16 [48, 3072, 1536], P('expert', None, 'tensor'), may hold values from -0.109375 to 0.109375
- w_down: bfloat16 [48, 1536, 3072], P('expert', 'tensor'), may hold values from -0.0625 to 0.0625
- expert_ids: int32 [3072, 2], P(('dp', 'expert')), may hold values from 0 to 7, as said below
- slots: int32 [3072, 2], P(('dp', 'expert')), may hold values from 0 to 3, as said below
Outputs:
- mixed: bfloat16 [3072, 3072], P(('dp', 'expert'))
- grad_tokens: bfloat16 [3072, 3072], P(('dp', 'expert'))
- grad_router: float32 [3072, 8], replicated
- grad_gain: float32 [3072], replicated
The draws below stay inside these ranges and needn't reach their ends.
Inputs may be any that keep to these rules, and one draw needn't show every extreme that they name: `expert_ids`: within each aligned block of 16 rows (one group), every expert is named exactly 4 times, and a row's two ids differ. Within each aligned block of 16 rows, the choices naming one expert hold its slots 0 to 3, each once.
All inputs are finite; a program needn't handle non-finite values.
Results may differ from the reference program's by a relative error of at most 0.0095.
Values may be sent and summed in bfloat16 or wider, within the bound.
A program may use at most 64 MiB of HBM per device.

```python
import jax
import jax.numpy as jnp
from jax import lax

D = 3072
FF = 9216
TOK_DEV = 16
SUBS = 6
EXPERTS = 8
CAP = 4
GROUPS = 192
TOKENS = 3072


def draw_tokens(key, part):
    base_key, row_key, column_key = jax.random.split(key, 3)
    base = jax.random.truncated_normal(base_key, -4.0, 4.0, (TOKENS, D), jnp.float32)
    row_scale = 10.0 ** jax.random.uniform(row_key, (TOKENS, 1), jnp.float32, -0.5, 0.5)
    column_scale = 10.0 ** jax.random.uniform(column_key, (1, D), jnp.float32, -0.5, 0.5)
    return (base * row_scale * column_scale).astype(jnp.bfloat16)


def group_routes(group_key):
    perm_key, shift_key, swap_key, rank_key = jax.random.split(group_key, 4)
    shuffled = jax.random.permutation(perm_key, TOK_DEV).astype(jnp.int32)
    first_ids = shuffled % EXPERTS
    round_index = shuffled // EXPERTS
    shift_by = jax.random.randint(shift_key, (TOK_DEV // EXPERTS,), 1, EXPERTS).astype(jnp.int32)
    second_ids = (first_ids + shift_by[round_index]) % EXPERTS
    swapped = jax.random.randint(swap_key, (TOK_DEV,), 0, 2).astype(jnp.int32)
    left = jnp.where(swapped == 1, second_ids, first_ids)
    right = jnp.where(swapped == 1, first_ids, second_ids)
    chosen_ids = jnp.stack([left, right], axis=1)
    ranking = jax.random.permutation(rank_key, 2 * TOK_DEV).astype(jnp.int32)
    flat_ids = chosen_ids.reshape(-1)
    same_expert = flat_ids[:, None] == flat_ids[None, :]
    earlier = ranking[None, :] < ranking[:, None]
    slot_ids = jnp.sum((same_expert & earlier).astype(jnp.int32), axis=1).reshape(TOK_DEV, 2)
    return (chosen_ids, slot_ids)


def route_tables(key):
    folded = jax.random.fold_in(key, 7)
    group_keys = jax.random.split(folded, TOKENS // TOK_DEV)
    chosen_ids, slot_ids = jax.vmap(group_routes)(group_keys)
    return (chosen_ids.reshape(TOKENS, 2).astype(jnp.int32), slot_ids.reshape(TOKENS, 2).astype(jnp.int32))


def draw_expert_ids(key, part):
    return route_tables(key)[0]


def draw_slots(key, part):
    return route_tables(key)[1]


def levels(own_key, dims, pieces, low, top_value):
    loudness = 1.0
    for dim, parts in pieces:
        steps = jax.random.uniform(jax.random.fold_in(jax.random.fold_in(own_key, 6), dim), (parts,), jnp.float32, low / len(pieces), top_value / len(pieces))
        loudness = loudness * jnp.repeat(jnp.exp(steps), dims[dim] // parts).reshape((-1,) + (1,) * (len(dims) - 1 - dim))
    return loudness


def scatter_about(rng, dims, spread, bound, cuts=(), held_as=jnp.bfloat16):
    result = jax.random.normal(rng, dims, jnp.float32) * spread
    if len(cuts) > 0:
        result = levels(rng, dims, cuts, -0.22, 0.18) * result
    return jnp.clip(result, min=-bound, max=bound).astype(held_as)


def setup_inputs(seed: int = 0) -> dict:
    streams_of = jax.random.split(jax.random.key(seed), 10)
    tokens = draw_tokens(jax.random.fold_in(streams_of[9], 71), 0)
    cotangent = scatter_about(streams_of[1], (TOKENS, D), 1.0, 6.0, ((0, 192),))
    gain = jnp.clip(1.0 + 0.1 * jax.random.normal(streams_of[2], (D,), jnp.float32), 0.5, 1.5)
    w_router = scatter_about(streams_of[3], (D, EXPERTS), D ** -0.5, 0.109375)
    w_gate = scatter_about(streams_of[4], (EXPERTS * SUBS, D, FF // SUBS), D ** -0.5, 0.109375, ((0, 48), (2, 4)))
    w_up = scatter_about(streams_of[5], (EXPERTS * SUBS, D, FF // SUBS), D ** -0.5, 0.109375, ((0, 48), (2, 4)))
    w_down = scatter_about(streams_of[6], (EXPERTS * SUBS, FF // SUBS, D), FF ** -0.5, 0.0625, ((0, 48), (1, 4)))
    expert_ids = draw_expert_ids(jax.random.fold_in(streams_of[9], 71), 0)
    slots = draw_slots(jax.random.fold_in(streams_of[9], 71), 0)
    return {"tokens": tokens, "cotangent": cotangent, "gain": gain, "w_router": w_router, "w_gate": w_gate, "w_up": w_up, "w_down": w_down, "expert_ids": expert_ids, "slots": slots}


epsilon = 1e-05

def reference(tokens, cotangent, gain, w_router, w_gate, w_up, w_down, expert_ids, slots):
    floats = tokens.astype(jnp.float32)
    inv_rms = lax.rsqrt(lax.optimization_barrier(jnp.mean(floats * floats, axis=1, keepdims=True)) + epsilon)
    normed = (floats * inv_rms * gain).astype(jnp.bfloat16)
    logits = jnp.dot(normed, w_router, preferred_element_type=jnp.float32)
    chosen_logits = jnp.take_along_axis(logits, expert_ids, axis=1)
    first_prob = jax.nn.sigmoid(chosen_logits[:, 0] - chosen_logits[:, 1])
    pair_probs = jnp.stack([first_prob, 1.0 - first_prob], axis=1)
    feature_width = tokens.shape[1]
    group_index = jnp.arange(TOKENS, dtype=jnp.int32) // TOK_DEV
    places = (group_index[:, None] * CAP + slots).astype(jnp.int32)
    expert_inputs = jnp.zeros((EXPERTS, GROUPS * CAP, feature_width), jnp.bfloat16)
    expert_inputs = expert_inputs.at[expert_ids, places].set(jnp.broadcast_to(normed[:, None, :], (TOKENS, 2, feature_width)))
    upstream = cotangent.astype(jnp.float32)
    sent_grads = (pair_probs[:, :, None] * upstream[:, None, :]).astype(jnp.bfloat16)
    expert_grads = jnp.zeros((EXPERTS, GROUPS * CAP, feature_width), jnp.bfloat16)
    expert_grads = expert_grads.at[expert_ids, places].set(sent_grads)
    hidden = w_gate.shape[2]
    gate_blocks = w_gate.reshape(EXPERTS, SUBS, feature_width, hidden)
    up_blocks = w_up.reshape(EXPERTS, SUBS, feature_width, hidden)
    down_blocks = w_down.reshape(EXPERTS, SUBS * hidden, feature_width)

    def one_expert(operand):
        rows_in, grads_in, gate_part, up_part, down_full = operand
        gate_full = jnp.transpose(gate_part, (1, 0, 2)).reshape(feature_width, SUBS * hidden)
        up_full = jnp.transpose(up_part, (1, 0, 2)).reshape(feature_width, SUBS * hidden)
        gate_pre = jnp.dot(rows_in, gate_full, preferred_element_type=jnp.float32)
        up_pre = jnp.dot(rows_in, up_full, preferred_element_type=jnp.float32)
        activated = (jax.nn.silu(gate_pre) * up_pre).astype(jnp.bfloat16)
        expert_out = jnp.dot(activated, down_full, preferred_element_type=jnp.float32)
        grad_act = jnp.dot(grads_in, down_full.T, preferred_element_type=jnp.float32)
        sigmoid_gate = jax.nn.sigmoid(gate_pre)
        grad_gate = (grad_act * up_pre * sigmoid_gate * (1.0 + gate_pre * (1.0 - sigmoid_gate))).astype(jnp.bfloat16)
        grad_up = (grad_act * jax.nn.silu(gate_pre)).astype(jnp.bfloat16)
        expert_back = jnp.dot(grad_gate, gate_full.T, preferred_element_type=jnp.float32) + jnp.dot(grad_up, up_full.T, preferred_element_type=jnp.float32)
        return (expert_out, expert_back)
    expert_out, expert_back = lax.map(one_expert, (expert_inputs, expert_grads, gate_blocks, up_blocks, down_blocks))
    chosen = expert_out[expert_ids, places]
    mixed = (floats + lax.optimization_barrier(jnp.sum(pair_probs[:, :, None] * chosen, axis=1))).astype(jnp.bfloat16)
    grad_mixture = lax.optimization_barrier(jnp.sum(expert_back[expert_ids, places], axis=1))
    grad_probs = lax.optimization_barrier(jnp.sum(upstream[:, None, :] * chosen, axis=2))
    grad_first = first_prob * (1.0 - first_prob) * (grad_probs[:, 0] - grad_probs[:, 1])
    columns = jnp.arange(EXPERTS, dtype=jnp.int32)[None, :]
    grad_logits = grad_first[:, None] * ((expert_ids[:, 0:1] == columns).astype(jnp.float32) - (expert_ids[:, 1:2] == columns).astype(jnp.float32))
    grad_router = jnp.dot(normed.astype(jnp.float32).T, grad_logits, precision=lax.Precision.HIGHEST)
    grad_normed = grad_mixture + jnp.dot(grad_logits, w_router.astype(jnp.float32).T, precision=lax.Precision.HIGHEST)
    grad_gain = lax.optimization_barrier(jnp.sum(grad_normed * floats * inv_rms, axis=0))
    grad_scaled = grad_normed * gain
    cubed = inv_rms * inv_rms * inv_rms
    grad_tokens = (upstream + inv_rms * grad_scaled - floats * cubed * lax.optimization_barrier(jnp.mean(grad_scaled * floats, axis=1, keepdims=True))).astype(jnp.bfloat16)
    return (mixed, grad_tokens, grad_router, grad_gain)
```

```python
import jax
import jax.numpy as jnp
from jax import lax
from jax.sharding import PartitionSpec as P

epsilon = 1e-05


def in_blocks(value, dim, devices):
    before, after = (value.shape[:dim], value.shape[dim + 1 :])
    return jnp.moveaxis(value.reshape(*before, devices, -1, *after), dim, 0)


def summed_on_arrival(value, axis, dim):
    parts = in_blocks(value, dim, lax.axis_size(axis))
    arrived = lax.all_to_all(parts, axis, split_axis=0, concat_axis=0, tiled=True)
    return arrived.astype(jnp.float32).sum(axis=0)


def in_one(arrays, axis):
    line, at, finished = (jnp.concatenate([a.reshape(-1) for a in arrays]), 0, [])
    quarter = line.size // lax.axis_size("tensor")
    owner = jnp.arange(line.size, dtype=jnp.int32) // quarter
    line = jnp.where(owner == lax.axis_index("tensor"), line, 0.0)
    so_far = lax.psum(line, axis)
    for a in arrays:
        finished.append(so_far[at : at + a.size].reshape(a.shape))
        at += a.size
    return tuple(finished)


def pack_rows(select, values):
    return jnp.einsum("tcr,tcd->rd", select, values, preferred_element_type=jnp.float32).astype(
        jnp.bfloat16
    )


def repeat_blocks(packed, experts, copies):
    feature_width = packed.shape[1]
    blocks = packed.reshape(experts, 1, -1, feature_width)
    blocks = jnp.broadcast_to(blocks, (experts, copies, blocks.shape[2], feature_width))
    return blocks.reshape(experts * copies, -1, feature_width)


def to_experts(packed, experts, copies):
    slice_width = packed.shape[1] // lax.axis_size("tensor")
    feature_slice = lax.dynamic_slice_in_dim(
        packed, lax.axis_index("tensor") * slice_width, slice_width, 1
    )
    arrived = lax.all_to_all(
        repeat_blocks(feature_slice, experts, copies),
        "expert",
        split_axis=0,
        concat_axis=0,
        tiled=True,
    )
    arrived = lax.all_gather(arrived, "tensor", axis=2, tiled=True)
    return arrived.reshape(-1, packed.shape[1])


def from_experts(partial_value, row_index, experts, copies):
    partial_value = summed_on_arrival(partial_value.astype(jnp.bfloat16), "tensor", 1)
    feature_width = partial_value.shape[1]
    returned_rows = lax.all_to_all(
        partial_value.astype(jnp.bfloat16).reshape(experts * copies, -1, feature_width),
        "expert",
        split_axis=0,
        concat_axis=0,
        tiled=True,
    ).astype(jnp.float32)
    summed = jnp.sum(returned_rows.reshape(experts, copies, -1, feature_width), axis=1).reshape(
        -1, feature_width
    )
    picked = summed[row_index]
    picked = lax.all_gather(picked.astype(jnp.bfloat16), "tensor", axis=2, tiled=True).astype(
        picked.dtype
    )
    return picked


def shards(tokens, cotangent, gain, w_router, w_gate, w_up, w_down, expert_ids, slots):
    experts = w_router.shape[1]
    copies = lax.axis_size("expert") // experts
    token_count = tokens.shape[0]
    capacity = 2 * token_count // experts
    floats = tokens.astype(jnp.float32)
    inv_rms = lax.rsqrt(jnp.mean(floats * floats, axis=1, keepdims=True) + epsilon)
    normed = (floats * inv_rms * gain).astype(jnp.bfloat16)
    logits = jnp.dot(normed, w_router, preferred_element_type=jnp.float32)
    chosen_logits = jnp.take_along_axis(logits, expert_ids, axis=1)
    first_prob = jax.nn.sigmoid(chosen_logits[:, 0] - chosen_logits[:, 1])
    pair_probs = jnp.stack([first_prob, 1.0 - first_prob], axis=1)
    row_index = expert_ids * capacity + slots
    select = (
        row_index[:, :, None] == jnp.arange(experts * capacity, dtype=jnp.int32)[None, None, :]
    ).astype(jnp.bfloat16)
    feature_width = tokens.shape[1]
    inputs = to_experts(
        pack_rows(select, jnp.broadcast_to(normed[:, None, :], (token_count, 2, feature_width))),
        experts,
        copies,
    )
    gate_matrix = w_gate[0]
    up_matrix = w_up[0]
    down_matrix = w_down[0]
    gate_pre = jnp.dot(inputs, gate_matrix, preferred_element_type=jnp.float32)
    up_pre = jnp.dot(inputs, up_matrix, preferred_element_type=jnp.float32)
    activated = (jax.nn.silu(gate_pre) * up_pre).astype(jnp.bfloat16)
    chosen = from_experts(
        jnp.dot(activated, down_matrix, preferred_element_type=jnp.float32),
        row_index,
        experts,
        copies,
    )
    mixed = (floats + jnp.sum(pair_probs[:, :, None] * chosen, axis=1)).astype(jnp.bfloat16)
    upstream = cotangent.astype(jnp.float32)
    sent_grads = (pair_probs[:, :, None] * upstream[:, None, :]).astype(jnp.bfloat16)
    grad_outputs = to_experts(pack_rows(select, sent_grads), experts, copies)
    grad_act = jnp.dot(grad_outputs, down_matrix.T, preferred_element_type=jnp.float32)
    sigmoid_gate = jax.nn.sigmoid(gate_pre)
    grad_gate = (grad_act * up_pre * sigmoid_gate * (1.0 + gate_pre * (1.0 - sigmoid_gate))).astype(
        jnp.bfloat16
    )
    grad_up = (grad_act * jax.nn.silu(gate_pre)).astype(jnp.bfloat16)
    grad_inputs = jnp.dot(grad_gate, gate_matrix.T, preferred_element_type=jnp.float32) + jnp.dot(
        grad_up, up_matrix.T, preferred_element_type=jnp.float32
    )
    grad_mixture = jnp.sum(from_experts(grad_inputs, row_index, experts, copies), axis=1)
    grad_probs = jnp.sum(upstream[:, None, :] * chosen, axis=2)
    grad_first = first_prob * (1.0 - first_prob) * (grad_probs[:, 0] - grad_probs[:, 1])
    columns = jnp.arange(experts, dtype=jnp.int32)[None, :]
    grad_logits = grad_first[:, None] * (
        (expert_ids[:, 0:1] == columns).astype(jnp.float32)
        - (expert_ids[:, 1:2] == columns).astype(jnp.float32)
    )
    grad_normed = grad_mixture + jnp.dot(
        grad_logits, w_router.astype(jnp.float32).T, precision=lax.Precision.HIGHEST
    )
    router_part = jnp.dot(
        normed.astype(jnp.float32).T, grad_logits, precision=lax.Precision.HIGHEST
    )
    gain_part = jnp.sum(grad_normed * floats * inv_rms, axis=0)
    grad_router, grad_gain = in_one((router_part, gain_part), ("dp", "expert", "tensor"))
    grad_scaled = grad_normed * gain
    cubed = inv_rms * inv_rms * inv_rms
    grad_tokens = (
        upstream
        + inv_rms * grad_scaled
        - floats * cubed * jnp.mean(grad_scaled * floats, axis=1, keepdims=True)
    ).astype(jnp.bfloat16)
    return (mixed, grad_tokens, grad_router, grad_gain)


def solution(mesh):
    return jax.shard_map(
        shards,
        mesh=mesh,
        in_specs=(
            P(("dp", "expert"), None),
            P(("dp", "expert"), None),
            P(),
            P(),
            P("expert", None, "tensor"),
            P("expert", None, "tensor"),
            P("expert", "tensor", None),
            P(("dp", "expert"), None),
            P(("dp", "expert"), None),
        ),
        out_specs=(P(("dp", "expert"), None), P(("dp", "expert"), None), P(), P()),
        check_vma=False,
    )
```

```python
import functools

import jax
import jax.numpy as jnp
from jax import lax
from jax.experimental import pallas as pl
from jax.experimental.pallas import tpu as pltpu
from jax.sharding import PartitionSpec as P

epsilon = 1e-05
LANES = 128
SLOTS = 4
LINE = 4
F32 = jnp.float32
BF16 = jnp.bfloat16
NT = (((1,), (1,)), ((), ()))


def low_rows(shape):
    return lax.broadcasted_iota(jnp.int32, shape, 1) < SLOTS


def split_rows(tiles):
    n = tiles.shape[0]
    pairs = tiles.reshape(n // 2, 2, 8, LANES)
    a, b = pairs[:, 0], pairs[:, 1]
    low = low_rows(a.shape)
    first = jnp.where(low, a, pltpu.roll(b, SLOTS, 1))
    second = jnp.where(low, pltpu.roll(a, SLOTS, 1), b)
    return first.reshape(4 * n, LANES), second.reshape(4 * n, LANES)


def join_rows(first, second):
    n = first.shape[0] // 4
    first = first.reshape(n // 2, 8, LANES)
    second = second.reshape(n // 2, 8, LANES)
    low = low_rows(first.shape)
    a = jnp.where(low, first, pltpu.roll(second, SLOTS, 1))
    b = jnp.where(low, pltpu.roll(first, SLOTS, 1), second)
    return jnp.concatenate([a[:, None], b[:, None]], axis=1).reshape(n, 8, LANES)


def layer_kernel(
    dims,
    tokens_ref, cot_ref, gain_ref, router_ref, sel0_ref, sel1_ref, selT0_ref, selT1_ref, sign_ref,
    gate_hbm, up_hbm, down_hbm,
    mixed_ref, gtok_ref, grouter_ref, ggain_ref,
    wg, wu, wd, packed, arrived, xin, gin, pre, hid, parts, fwd_in, left_in, right_in, reduced,
    copy_in, finished, back, mixed_all, gtok_all, scal_out, scal_in, sums, line_in, line_sum,
    z_in, z_sum, grads,
    w_sem, a2a_sem, cp_send, cp_recv, xl_send, xr_send, xf_send, xl_recv, xr_recv, xf_recv,
    f_send, f_recv, l_send, r_send, l_recv, r_recv, c_send, c_recv, back_sem,
    sc_send, sc_recv, mx_send, mx_recv, gt_send, gt_recv, line_sem, z_sem, gl_sem, gx_send, gx_recv,
):
    n_dp, n_e, n_t, experts, copies = dims
    width = copies * LANES
    half = copies // 2
    d, e, t = lax.axis_index("dp"), lax.axis_index("expert"), lax.axis_index("tensor")
    k, s = e // copies, e % copies
    z, line = e // LINE, d * LINE + e % LINE
    n_z, n_line = n_e // LINE, n_dp * LINE
    left, right, across = (t + n_t - 1) % n_t, (t + 1) % n_t, (t + 2) % n_t
    mine = t * copies + s
    sl = pl.ds(pl.multiple_of(t * width, LANES), width)

    def place(dp, expert, tensor):
        return (dp, expert, tensor)

    def remote(src, dst, send, recv, target):
        return pltpu.make_async_remote_copy(
            src_ref=src, dst_ref=dst, send_sem=send, recv_sem=recv,
            device_id=target, device_id_type=pl.DeviceIdType.MESH,
        )

    weights = [
        pltpu.make_async_copy(a, b, w_sem.at[i])
        for i, (a, b) in enumerate(((gate_hbm, wg), (up_hbm, wu), (down_hbm, wd)))
    ]
    for w in weights:
        w.start()

    bar = pltpu.get_barrier_semaphore()

    @pl.loop(1, n_e)
    def _(i):
        pl.semaphore_signal(bar, inc=1, device_id=place(d, (e + i) % n_e, t),
                            device_id_type=pl.DeviceIdType.MESH)

    for o in range(1, n_t):
        pl.semaphore_signal(bar, inc=1, device_id=place(d, e, (t + o) % n_t),
                            device_id_type=pl.DeviceIdType.MESH)

    @pl.loop(0, (n_dp - 1) * LINE)
    def _(i):
        pl.semaphore_signal(
            bar, inc=1, device_id=place((d + 1 + i // LINE) % n_dp, z * LINE + i % LINE, t),
            device_id_type=pl.DeviceIdType.MESH)

    floats = tokens_ref[...].astype(F32)
    inv_rms = lax.rsqrt(jnp.mean(floats * floats, axis=1, keepdims=True) + epsilon)
    normed = (floats * inv_rms * gain_ref[...]).astype(BF16)
    logits = lax.dot_general(normed, router_ref[...], NT, preferred_element_type=F32)
    sign = sign_ref[...]
    p0 = jax.nn.sigmoid(jnp.sum(logits * sign, axis=1, keepdims=True))
    p1 = 1.0 - p0
    toks = tokens_ref[:, sl].astype(F32)
    cots = cot_ref[:, sl].astype(F32)
    gains = gain_ref[:, sl]
    normeds = (toks * inv_rms * gains).astype(BF16)
    selT0, selT1 = selT0_ref[...], selT1_ref[...]
    rows_in = jnp.dot(selT0 + selT1, normeds, preferred_element_type=F32)
    rows_g = (jnp.dot(selT0, (p0 * cots).astype(BF16), preferred_element_type=F32)
              + jnp.dot(selT1, (p1 * cots).astype(BF16), preferred_element_type=F32))
    for c in range(copies):
        at = slice(c * LANES, (c + 1) * LANES)
        packed[:, c] = join_rows(rows_in[:, at], rows_g[:, at]).astype(BF16)

    pl.semaphore_wait(bar, n_e - 1 + n_t - 1 + (n_dp - 1) * LINE)

    @pl.loop(1, n_e)
    def _(i):
        to = (e + i) % n_e
        remote(packed.at[to // copies, to % copies], arrived.at[t * copies + to % copies, e],
               a2a_sem.at[0], a2a_sem.at[1], place(d, to, t)).start()

    arrived[mine, e] = packed[k, s]
    scaled = floats * gain_ref[...]
    router = router_ref[...].astype(F32)
    through = jnp.concatenate(
        [jnp.sum(scaled * router[j : j + 1], axis=1, keepdims=True) for j in range(experts)], axis=1)

    a2a = remote(arrived.at[mine, pl.ds(0, n_e - 1)], arrived.at[mine, pl.ds(0, n_e - 1)],
                 a2a_sem.at[0], a2a_sem.at[1], place(d, e, right))
    a2a.wait_recv()

    def piece(i):
        return (s + i) % copies

    started = []

    def go(copy):
        copy.start()
        started.append(copy)

    for i in range(1, copies):
        go(remote(arrived.at[mine], arrived.at[mine], cp_send.at[i], cp_recv.at[s],
                  place(d, k * copies + piece(i), t)))

    def chunk(tensor, i):
        return arrived.at[tensor * copies + piece(i)]

    def from_left(i):
        remote(chunk(left, i), chunk(left, i), xr_send.at[i], xr_recv.at[i], place(d, e, right)).wait_recv()

    def from_right(i):
        remote(chunk(right, i), chunk(right, i), xl_send.at[i], xl_recv.at[i], place(d, e, left)).wait_recv()

    def pass_on(i):
        from_left(i)
        from_right(i)
        if i < half:
            go(remote(chunk(left, i), chunk(left, i), xf_send.at[i], xf_recv.at[i], place(d, e, right)))
        else:
            go(remote(chunk(right, i), chunk(right, i), xf_send.at[i], xf_recv.at[i], place(d, e, left)))

    for i in range(copies):
        if i > 0:
            remote(chunk(t, i), chunk(t, i), cp_send.at[i], cp_recv.at[piece(i)], place(d, e, right)).wait_recv()
        go(remote(chunk(t, i), chunk(t, i), xr_send.at[i], xr_recv.at[i], place(d, e, right)))
        go(remote(chunk(t, i), chunk(t, i), xl_send.at[i], xl_recv.at[i], place(d, e, left)))
        if i > 0:
            pass_on(i - 1)
    pass_on(copies - 1)

    pre[...] = jnp.zeros_like(pre)
    for w in weights:
        w.wait()

    def features(q):
        for c in range(copies):
            first, second = split_rows(arrived[q * copies + c].astype(F32))
            at = slice(c * LANES, (c + 1) * LANES)
            xin[:, at] = first.astype(BF16)
            gin[:, at] = second.astype(BF16)
        x, g = xin[...], gin[...]
        pre[0] += jnp.dot(x, wg[q], preferred_element_type=F32)
        pre[1] += jnp.dot(x, wu[q], preferred_element_type=F32)
        down = wd[:, pl.ds(pl.multiple_of(q * width, LANES), width)]
        pre[2] += lax.dot_general(g, down, NT, preferred_element_type=F32)

    @pl.loop(0, n_t - 1)
    def _(j):
        features((t + jnp.where(j == 2, 3, j)) % n_t)

    for i in range(copies):
        remote(chunk(across, i), chunk(across, i), xf_send.at[i], xf_recv.at[i],
               place(d, e, right)).wait_recv()
    features(across)

    gate, up, grad_act = pre[0], pre[1], pre[2]
    sig = jax.nn.sigmoid(gate)
    silu = gate * sig
    hid[0] = (silu * up).astype(BF16)
    hid[1] = (grad_act * up * sig * (1.0 + gate * (1.0 - sig))).astype(BF16)
    hid[2] = (grad_act * silu).astype(BF16)

    def quarter(q):
        down = wd[:, pl.ds(pl.multiple_of(q * width, LANES), width)]
        y = jnp.dot(hid[0], down, preferred_element_type=F32)
        g = (lax.dot_general(hid[1], wg[q], NT, preferred_element_type=F32)
             + lax.dot_general(hid[2], wu[q], NT, preferred_element_type=F32))
        for c in range(copies):
            at = slice(c * LANES, (c + 1) * LANES)
            parts[q, c] = join_rows(y[:, at], g[:, at]).astype(BF16)

    order = [(i + 1) % copies for i in range(copies)]
    quarter(across)
    for i in order:
        src = parts.at[across, piece(i)]
        go(remote(src, fwd_in.at[i], f_send.at[i], f_recv.at[i], place(d, e, right if i < half else left)))

    @pl.loop(0, 3)
    def _(j):
        quarter((t + jnp.where(j == 0, 1, jnp.where(j == 1, n_t - 1, 0))) % n_t)

    for i in order:
        remote(fwd_in.at[i], fwd_in.at[i], f_send.at[i], f_recv.at[i], place(d, e, right)).wait_recv()
        on = right if i < half else left
        parts[on, piece(i)] = (parts[on, piece(i)].astype(F32) + fwd_in[i].astype(F32)).astype(BF16)
        go(remote(parts.at[right, piece(i)], left_in.at[i], r_send.at[i], r_recv.at[i], place(d, e, right)))
        go(remote(parts.at[left, piece(i)], right_in.at[i], l_send.at[i], l_recv.at[i], place(d, e, left)))

    for i in order:
        remote(left_in.at[i], left_in.at[i], r_send.at[i], r_recv.at[i], place(d, e, right)).wait_recv()
        remote(right_in.at[i], right_in.at[i], l_send.at[i], l_recv.at[i], place(d, e, left)).wait_recv()
        total = parts[t, piece(i)].astype(F32) + left_in[i].astype(F32) + right_in[i].astype(F32)
        reduced[i] = total.astype(BF16)
        if i > 0:
            go(remote(reduced.at[i], copy_in.at[i], c_send.at[i], c_recv.at[i],
                      place(d, k * copies + piece(i), t)))
    total = reduced[0].astype(F32)
    for i in range(1, copies):
        remote(copy_in.at[i], copy_in.at[i], c_send.at[i], c_recv.at[i], place(d, e, right)).wait_recv()
        total = total + copy_in[i].astype(F32)
    finished[...] = total.astype(BF16)

    @pl.loop(1, n_e)
    def _(i):
        to = (e + i) % n_e
        remote(finished.at[to], back.at[k, s], back_sem.at[0], back_sem.at[1], place(d, to, t)).start()

    back[k, s] = finished[e]
    bulk = arrived.at[0, pl.ds(0, n_e - 1)]
    back_bulk = remote(bulk, bulk, back_sem.at[0], back_sem.at[1], place(d, e, right))
    back_bulk.wait_recv()

    ys, gs = [], []
    for c in range(copies):
        first, second = split_rows(back[:, c].astype(F32))
        ys.append(first.astype(BF16))
        gs.append(second.astype(BF16))
    y, g = jnp.concatenate(ys, axis=1), jnp.concatenate(gs, axis=1)
    sel0, sel1 = sel0_ref[...], sel1_ref[...]
    chosen0 = jnp.dot(sel0, y, preferred_element_type=F32)
    chosen1 = jnp.dot(sel1, y, preferred_element_type=F32)
    grad_mix = jnp.dot(sel0 + sel1, g, preferred_element_type=F32)
    rows = toks.shape[0]
    diff = jnp.sum(cots * (chosen0 - chosen1), axis=1, keepdims=True)
    dots = jnp.sum(grad_mix * gains * toks, axis=1, keepdims=True)
    column = lax.broadcasted_iota(jnp.int32, (rows, LANES), 1)
    scal_out[...] = jnp.where(column == 0, diff, jnp.where(column == 1, dots, 0.0))
    mixed_all[t] = (toks + (p0 * chosen0 + p1 * chosen1)).astype(BF16)
    for o in range(1, n_t):
        go(remote(scal_out, scal_in.at[o - 1], sc_send.at[o - 1], sc_recv.at[o - 1], place(d, e, (t + o) % n_t)))
    for o in range(1, n_t):
        go(remote(mixed_all.at[t], mixed_all.at[t], mx_send.at[o - 1], mx_recv.at[o - 1],
                  place(d, e, (t + o) % n_t)))
    scalars = scal_out[...]
    for o in range(1, n_t):
        remote(scal_in.at[o - 1], scal_in.at[o - 1], sc_send.at[o - 1], sc_recv.at[o - 1],
               place(d, e, right)).wait_recv()
        scalars = scalars + scal_in[o - 1]
    grad_first = p0 * p1 * scalars[:, 0:1]
    grad_logits = grad_first * sign
    grad_normed = grad_mix
    routers = router_ref[:, sl].astype(F32)
    for j in range(experts):
        grad_normed = grad_normed + grad_logits[:, j : j + 1] * routers[j : j + 1]
    normed32 = normeds.astype(F32)
    router_part = jnp.concatenate(
        [jnp.sum(grad_logits[:, j : j + 1] * normed32, axis=0, keepdims=True) for j in range(experts)], axis=0)
    gain_part = jnp.sum(grad_normed * toks * inv_rms, axis=0, keepdims=True)
    units = sums.shape[1]

    def unit(u):
        return u // units, u % units

    n_half = experts // SLOTS
    for c in range(copies):
        at = slice(c * LANES, (c + 1) * LANES)
        for h in range(n_half):
            a, b = unit(c * n_half + h)
            sums[a, b] = router_part[h * SLOTS : (h + 1) * SLOTS, at]
        a, b = unit(n_half * copies + c // SLOTS)
        sums[a, b, c % SLOTS : c % SLOTS + 1] = gain_part[:, at]

    def member(i):
        j = (line + i) % n_line
        return j, place(j // LINE, z * LINE + j % LINE, t)

    @pl.loop(1, n_line)
    def _(i):
        j, target = member(i)
        remote(sums.at[j], line_in.at[line], line_sem.at[0], line_sem.at[1], target).start()

    mean = (scalars[:, 1:2] + jnp.sum(grad_logits * through, axis=1, keepdims=True)) / (n_t * width)
    cubed = inv_rms * inv_rms * inv_rms
    gtok_all[t] = (cots + inv_rms * (grad_normed * gains) - toks * cubed * mean).astype(BF16)
    for o in range(1, n_t):
        go(remote(gtok_all.at[t], gtok_all.at[t], gt_send.at[o - 1], gt_recv.at[o - 1],
                  place(d, e, (t + o) % n_t)))
    line_in[line] = sums[line]
    some = pl.ds(0, n_line - 1)
    line_bulk = remote(line_in.at[some], line_in.at[some], line_sem.at[0], line_sem.at[1], place(d, e, right))
    line_bulk.wait_recv()
    line_sum[...] = jnp.sum(line_in[...], axis=0)

    if n_z > 1:
        @pl.loop(1, n_z)
        def _(i):
            to = (z + i) % n_z
            remote(line_sum, z_in.at[z], z_sem.at[0], z_sem.at[1], place(d, to * LINE + e % LINE, t)).start()

        z_in[z] = line_sum[...]
        zs = pl.ds(0, n_z - 1)
        z_bulk = remote(z_in.at[zs], z_in.at[zs], z_sem.at[0], z_sem.at[1], place(d, e, right))
        z_bulk.wait_recv()
        z_sum[...] = jnp.sum(z_in[...], axis=0)
    else:
        z_sum[...] = line_sum[...]

    @pl.loop(1, n_line)
    def _(i):
        j, target = member(i)
        remote(z_sum, grads.at[t, line], gl_sem.at[0], gl_sem.at[1], target).start()

    grads[t, line] = z_sum[...]
    gl_bulk = remote(grads.at[t, some], grads.at[t, some], gl_sem.at[0], gl_sem.at[1], place(d, e, right))
    gl_bulk.wait_recv()
    for o in range(1, n_t):
        go(remote(grads.at[t], grads.at[t], gx_send.at[o - 1], gx_recv.at[o - 1], place(d, e, (t + o) % n_t)))

    def other(o):
        return (t + n_t - o) % n_t

    for o in range(1, n_t):
        remote(mixed_all.at[other(o)], mixed_all.at[other(o)], mx_send.at[o - 1], mx_recv.at[o - 1],
               place(d, e, right)).wait_recv()
        remote(gtok_all.at[other(o)], gtok_all.at[other(o)], gt_send.at[o - 1], gt_recv.at[o - 1],
               place(d, e, right)).wait_recv()
    for q in range(n_t):
        at = slice(q * width, (q + 1) * width)
        mixed_ref[:, at] = mixed_all[q]
        gtok_ref[:, at] = gtok_all[q]
    for o in range(1, n_t):
        remote(grads.at[other(o)], grads.at[other(o)], gx_send.at[o - 1], gx_recv.at[o - 1],
               place(d, e, right)).wait_recv()
    for q in range(n_t):
        for c in range(copies):
            at = slice(q * width + c * LANES, q * width + (c + 1) * LANES)
            for h in range(n_half):
                a, b = unit(c * n_half + h)
                grouter_ref[h * SLOTS : (h + 1) * SLOTS, at] = grads[q, a, b]
            a, b = unit(n_half * copies + c // SLOTS)
            ggain_ref[:, at] = grads[q, a, b, c % SLOTS : c % SLOTS + 1]

    a2a.wait_send()
    back_bulk.wait_send()
    line_bulk.wait_send()
    if n_z > 1:
        z_bulk.wait_send()
    gl_bulk.wait_send()
    for copy in started:
        copy.wait_send()


def shards(dims, tokens, cotangent, gain, w_router, w_gate, w_up, w_down, expert_ids, slots):
    n_dp, n_e, n_t, experts, copies = dims
    count, features = tokens.shape
    hidden = w_gate.shape[2]
    width = features // n_t
    n_rows = n_e * SLOTS
    n_line, n_z = n_dp * LINE, n_e // LINE
    row_index = expert_ids * SLOTS + slots
    tile = jnp.arange(experts * SLOTS, dtype=jnp.int32)
    sel = [(row_index[:, c : c + 1] == tile[None, :]).astype(BF16) for c in range(2)]
    sel_t = [(row_index[:, c][None, :] == tile[:, None]).astype(BF16) for c in range(2)]
    columns = jnp.arange(experts, dtype=jnp.int32)[None, :]
    sign = (expert_ids[:, 0:1] == columns).astype(F32) - (expert_ids[:, 1:2] == columns).astype(F32)
    units = -(-(copies * (experts // SLOTS) + -(-copies // SLOTS)) // n_line)
    block = (n_e, 8, LANES)
    dma = pltpu.SemaphoreType.DMA
    vmem = pl.BlockSpec(memory_space=pltpu.VMEM)
    scratch = [
        pltpu.VMEM((n_t, width, hidden), BF16), pltpu.VMEM((n_t, width, hidden), BF16),
        pltpu.VMEM((hidden, features), BF16),
        pltpu.VMEM((experts, copies, 8, LANES), BF16),
        pltpu.VMEM((n_t * copies,) + block, BF16),
        pltpu.VMEM((n_rows, width), BF16), pltpu.VMEM((n_rows, width), BF16),
        pltpu.VMEM((3, n_rows, hidden), F32), pltpu.VMEM((3, n_rows, hidden), BF16),
        pltpu.VMEM((n_t, copies) + block, BF16),
        pltpu.VMEM((copies,) + block, BF16), pltpu.VMEM((copies,) + block, BF16),
        pltpu.VMEM((copies,) + block, BF16), pltpu.VMEM((copies,) + block, BF16),
        pltpu.VMEM((copies,) + block, BF16),
        pltpu.VMEM(block, BF16),
        pltpu.VMEM((experts, copies, 8, LANES), BF16),
        pltpu.VMEM((n_t, count, width), BF16), pltpu.VMEM((n_t, count, width), BF16),
        pltpu.VMEM((count, LANES), F32), pltpu.VMEM((n_t - 1, count, LANES), F32),
        pltpu.VMEM((n_line, units, SLOTS, LANES), F32), pltpu.VMEM((n_line, units, SLOTS, LANES), F32),
        pltpu.VMEM((units, SLOTS, LANES), F32),
        pltpu.VMEM((n_z, units, SLOTS, LANES), F32), pltpu.VMEM((units, SLOTS, LANES), F32),
        pltpu.VMEM((n_t, n_line, units, SLOTS, LANES), F32),
        dma((3,)), dma((2,)),
    ] + [dma((copies,))] * 16 + [dma((2,))] + [dma((n_t - 1,))] * 6 + [dma((2,))] * 3 + [dma((n_t - 1,))] * 2
    mixed, gtok, grouter, ggain = pl.pallas_call(
        functools.partial(layer_kernel, dims),
        out_shape=(
            jax.ShapeDtypeStruct((count, features), BF16), jax.ShapeDtypeStruct((count, features), BF16),
            jax.ShapeDtypeStruct((experts, features), F32), jax.ShapeDtypeStruct((1, features), F32),
        ),
        in_specs=[vmem] * 9 + [pl.BlockSpec(memory_space=pl.ANY)] * 3,
        out_specs=(vmem,) * 4,
        scratch_shapes=scratch,
        compiler_params=pltpu.CompilerParams(
            collective_id=0, has_side_effects=True, vmem_limit_bytes=56 * 1024 * 1024),
    )(
        tokens, cotangent, gain.reshape(1, features), w_router.T, sel[0], sel[1], sel_t[0], sel_t[1], sign,
        w_gate.reshape(n_t, width, hidden), w_up.reshape(n_t, width, hidden), w_down.reshape(hidden, features),
    )
    return mixed, gtok, grouter.T, ggain.reshape(features)


def solution(mesh):
    n_dp, n_e, n_t = (mesh.shape[a] for a in ("dp", "expert", "tensor"))

    def body(*args):
        experts = args[3].shape[1]
        return shards((n_dp, n_e, n_t, experts, n_e // experts), *args)

    return jax.shard_map(
        body,
        mesh=mesh,
        in_specs=(
            P(("dp", "expert"), None),
            P(("dp", "expert"), None),
            P(),
            P(),
            P("expert", None, "tensor"),
            P("expert", None, "tensor"),
            P("expert", "tensor", None),
            P(("dp", "expert"), None),
            P(("dp", "expert"), None),
        ),
        out_specs=(P(("dp", "expert"), None), P(("dp", "expert"), None), P(), P()),
        check_vma=False,
    )
```

```python
import functools

import jax
import jax.numpy as jnp
from jax import lax
from jax.experimental import pallas as pl
from jax.experimental.pallas import tpu as pltpu
from jax.sharding import PartitionSpec as P

epsilon = 1e-05
LANES = 128
SLOTS = 4
LINE = 4
BANDS = 3
LAG = 3
AHEAD = 2
F32 = jnp.float32
BF16 = jnp.bfloat16
NT = (((1,), (1,)), ((), ()))


def low_rows(shape):
    return lax.broadcasted_iota(jnp.int32, shape, 1) < SLOTS


def split_rows(tiles):
    n = tiles.shape[0]
    pairs = tiles.reshape(n // 2, 2, 8, LANES)
    a, b = pairs[:, 0], pairs[:, 1]
    low = low_rows(a.shape)
    first = jnp.where(low, a, pltpu.roll(b, SLOTS, 1))
    second = jnp.where(low, pltpu.roll(a, SLOTS, 1), b)
    return first.reshape(4 * n, LANES), second.reshape(4 * n, LANES)


def join_rows(first, second):
    n = first.shape[0] // 4
    first = first.reshape(n // 2, 8, LANES)
    second = second.reshape(n // 2, 8, LANES)
    low = low_rows(first.shape)
    a = jnp.where(low, first, pltpu.roll(second, SLOTS, 1))
    b = jnp.where(low, pltpu.roll(first, SLOTS, 1), second)
    return jnp.concatenate([a[:, None], b[:, None]], axis=1).reshape(n, 8, LANES)


def one_hots(ids, slots, experts):
    count, n_rows = ids.shape[1], experts * SLOTS
    rows = ids * SLOTS + slots
    at = lax.broadcasted_iota(jnp.int32, (n_rows, count), 0)
    picks = [(at == rows[c : c + 1]).astype(F32) for c in range(2)]
    expert = lax.broadcasted_iota(jnp.int32, (experts, count), 0)
    signs = (expert == ids[0:1]).astype(F32) - (expert == ids[1:2]).astype(F32)
    both = jnp.concatenate(picks + [signs], axis=0)
    fill = -both.shape[0] % LANES
    both = jnp.concatenate([both, jnp.zeros((fill, count), F32)], axis=0)
    both = jnp.concatenate([both, jnp.zeros((both.shape[0], LANES - count), F32)], axis=1)
    turned = both.T
    sel0 = turned[:count, :n_rows].astype(BF16)
    sel1 = turned[:count, n_rows : 2 * n_rows].astype(BF16)
    sign = turned[:count, 2 * n_rows : 2 * n_rows + experts]
    return sel0, sel1, sign, picks[0].astype(BF16), picks[1].astype(BF16)


def layer_kernel(
    dims,
    tokens_ref, cot_ref, gain_ref, router_ref, ids_ref, slots_ref,
    gate_hbm, up_hbm, down_hbm,
    mixed_all, gtok_all, grads,
    wg, wu, wd, packed, arrived, xin, gin, pre, hid, parts, fwd_in, left_in, right_in, reduced,
    copy_in, finished, back, scal_out, scal_in, sums, line_in, line_sum, z_in, z_sum,
    w_sem, a2a_sem, cp_send, cp_recv, xl_send, xr_send, xf_send, xl_recv, xr_recv, xf_recv,
    f_send, f_recv, l_send, r_send, l_recv, r_recv, c_send, c_recv, back_sem,
    sc_send, sc_recv, mx_send, mx_recv, gt_send, gt_recv, line_sem, z_sem, gl_sem, gx_send, gx_recv,
):
    n_dp, n_e, n_t, experts, copies = dims
    width = copies * LANES
    half = copies // 2
    d, e, t = lax.axis_index("dp"), lax.axis_index("expert"), lax.axis_index("tensor")
    k, s = e // copies, e % copies
    z, line = e // LINE, d * LINE + e % LINE
    n_z, n_line = n_e // LINE, n_dp * LINE
    left, right, across = (t + n_t - 1) % n_t, (t + 1) % n_t, (t + 2) % n_t
    mine = t * copies + s
    sl = pl.ds(pl.multiple_of(t * width, LANES), width)

    def place(dp, expert, tensor):
        return (dp, expert, tensor)

    def remote(src, dst, send, recv, target):
        return pltpu.make_async_remote_copy(
            src_ref=src, dst_ref=dst, send_sem=send, recv_sem=recv,
            device_id=target, device_id_type=pl.DeviceIdType.MESH,
        )

    weights = [
        pltpu.make_async_copy(a, b, w_sem.at[i])
        for i, (a, b) in enumerate(((gate_hbm, wg), (up_hbm, wu), (down_hbm, wd)))
    ]
    for w in weights:
        w.start()

    bar = pltpu.get_barrier_semaphore()

    @pl.loop(1, n_e)
    def _(i):
        pl.semaphore_signal(bar, inc=1, device_id=place(d, (e + i) % n_e, t),
                            device_id_type=pl.DeviceIdType.MESH)

    for o in range(1, n_t):
        pl.semaphore_signal(bar, inc=1, device_id=place(d, e, (t + o) % n_t),
                            device_id_type=pl.DeviceIdType.MESH)

    @pl.loop(0, (n_dp - 1) * LINE)
    def _(i):
        pl.semaphore_signal(
            bar, inc=1, device_id=place((d + 1 + i // LINE) % n_dp, z * LINE + i % LINE, t),
            device_id_type=pl.DeviceIdType.MESH)

    floats = tokens_ref[...].astype(F32)
    inv_rms = lax.rsqrt(jnp.mean(floats * floats, axis=1, keepdims=True) + epsilon)
    normed = (floats * inv_rms * gain_ref[...]).astype(BF16)
    logits = lax.dot_general(normed, router_ref[...], NT, preferred_element_type=F32)
    sel0, sel1, sign, selT0, selT1 = one_hots(ids_ref[...], slots_ref[...], experts)
    p0 = jax.nn.sigmoid(jnp.sum(logits * sign, axis=1, keepdims=True))
    p1 = 1.0 - p0
    toks = tokens_ref[:, sl].astype(F32)
    cots = cot_ref[:, sl].astype(F32)
    gains = gain_ref[:, sl]
    normeds = (toks * inv_rms * gains).astype(BF16)
    rows_in = jnp.dot(selT0 + selT1, normeds, preferred_element_type=F32)
    rows_g = (jnp.dot(selT0, (p0 * cots).astype(BF16), preferred_element_type=F32)
              + jnp.dot(selT1, (p1 * cots).astype(BF16), preferred_element_type=F32))
    for c in range(copies):
        at = slice(c * LANES, (c + 1) * LANES)
        packed[:, c] = join_rows(rows_in[:, at], rows_g[:, at]).astype(BF16)

    pl.semaphore_wait(bar, n_e - 1 + n_t - 1 + (n_dp - 1) * LINE)

    @pl.loop(1, n_e)
    def _(i):
        to = (e + i) % n_e
        remote(packed.at[to // copies, to % copies], arrived.at[t * copies + to % copies, e],
               a2a_sem.at[0], a2a_sem.at[1], place(d, to, t)).start()

    arrived[mine, e] = packed[k, s]
    scaled = floats * gain_ref[...]
    router = router_ref[...].astype(F32)
    through = jnp.concatenate(
        [jnp.sum(scaled * router[j : j + 1], axis=1, keepdims=True) for j in range(experts)], axis=1)

    a2a = remote(arrived.at[mine, pl.ds(0, n_e - 1)], arrived.at[mine, pl.ds(0, n_e - 1)],
                 a2a_sem.at[0], a2a_sem.at[1], place(d, e, right))
    a2a.wait_recv()

    def piece(i):
        return (s + i) % copies

    started = []

    def go(copy):
        copy.start()
        started.append(copy)

    bands = cp_send.shape[1]
    span = n_e // bands

    def band(tensor, i, h):
        return arrived.at[tensor * copies + piece(i), pl.ds(h * span, span)]

    def arrives(block, recv):
        remote(block, block, cp_send.at[0, 0], recv, place(d, e, right)).wait_recv()

    def to_copies(h):
        for i in range(1, copies):
            own = band(t, 0, h)
            go(remote(own, own, cp_send.at[i, h], cp_recv.at[s, h], place(d, k * copies + piece(copies - i), t)))

    to_copies(0)

    def both_ways(i, h):
        block = band(t, i, h)
        go(remote(block, block, xr_send.at[i, h], xr_recv.at[i, h], place(d, e, right)))
        go(remote(block, block, xl_send.at[i, h], xl_recv.at[i, h], place(d, e, left)))

    def pass_on(i, h):
        arrives(band(left, i, h), xr_recv.at[i, h])
        arrives(band(right, i, h), xl_recv.at[i, h])
        block, to = (band(left, i, h), right) if i < half else (band(right, i, h), left)
        go(remote(block, block, xf_send.at[i, h], xf_recv.at[i, h], place(d, e, to)))

    steps = [(i, h) for h in range(bands) for i in range(copies)]
    waiting = []
    for i, h in steps:
        if i > 0:
            arrives(band(t, i, h), cp_recv.at[piece(i), h])
        both_ways(i, h)
        if i == AHEAD and h + 1 < bands:
            to_copies(h + 1)
        waiting.append((i, h))
        if len(waiting) > LAG:
            pass_on(*waiting.pop(0))
    for i, h in waiting:
        pass_on(i, h)

    pre[...] = jnp.zeros_like(pre)
    for w in weights:
        w.wait()

    def features(q):
        for c in range(copies):
            first, second = split_rows(arrived[q * copies + c].astype(F32))
            at = slice(c * LANES, (c + 1) * LANES)
            xin[:, at] = first.astype(BF16)
            gin[:, at] = second.astype(BF16)
        x, g = xin[...], gin[...]
        pre[0] += jnp.dot(x, wg[q], preferred_element_type=F32)
        pre[1] += jnp.dot(x, wu[q], preferred_element_type=F32)
        down = wd[:, pl.ds(pl.multiple_of(q * width, LANES), width)]
        pre[2] += lax.dot_general(g, down, NT, preferred_element_type=F32)

    @pl.loop(0, n_t - 1)
    def _(j):
        features((t + jnp.where(j == 2, 3, j)) % n_t)

    for i, h in steps:
        arrives(band(across, i, h), xf_recv.at[i, h])
    features(across)

    gate, up, grad_act = pre[0], pre[1], pre[2]
    sig = jax.nn.sigmoid(gate)
    silu = gate * sig
    hid[0] = (silu * up).astype(BF16)
    hid[1] = (grad_act * up * sig * (1.0 + gate * (1.0 - sig))).astype(BF16)
    hid[2] = (grad_act * silu).astype(BF16)

    def quarter(q):
        down = wd[:, pl.ds(pl.multiple_of(q * width, LANES), width)]
        y = jnp.dot(hid[0], down, preferred_element_type=F32)
        g = (lax.dot_general(hid[1], wg[q], NT, preferred_element_type=F32)
             + lax.dot_general(hid[2], wu[q], NT, preferred_element_type=F32))
        for c in range(copies):
            at = slice(c * LANES, (c + 1) * LANES)
            parts[q, c] = join_rows(y[:, at], g[:, at]).astype(BF16)

    order = [(i + 1) % copies for i in range(copies)]
    quarter(across)
    for i in order:
        src = parts.at[across, piece(i)]
        go(remote(src, fwd_in.at[i], f_send.at[i], f_recv.at[i], place(d, e, right if i < half else left)))

    @pl.loop(0, 3)
    def _(j):
        quarter((t + jnp.where(j == 0, 1, jnp.where(j == 1, n_t - 1, 0))) % n_t)

    for i in order:
        remote(fwd_in.at[i], fwd_in.at[i], f_send.at[i], f_recv.at[i], place(d, e, right)).wait_recv()
        on = right if i < half else left
        parts[on, piece(i)] = (parts[on, piece(i)].astype(F32) + fwd_in[i].astype(F32)).astype(BF16)
        go(remote(parts.at[right, piece(i)], left_in.at[i], r_send.at[i], r_recv.at[i], place(d, e, right)))
        go(remote(parts.at[left, piece(i)], right_in.at[i], l_send.at[i], l_recv.at[i], place(d, e, left)))

    for i in order:
        remote(left_in.at[i], left_in.at[i], r_send.at[i], r_recv.at[i], place(d, e, right)).wait_recv()
        remote(right_in.at[i], right_in.at[i], l_send.at[i], l_recv.at[i], place(d, e, left)).wait_recv()
        total = parts[t, piece(i)].astype(F32) + left_in[i].astype(F32) + right_in[i].astype(F32)
        reduced[i] = total.astype(BF16)
        if i > 0:
            go(remote(reduced.at[i], copy_in.at[i], c_send.at[i], c_recv.at[i],
                      place(d, k * copies + piece(i), t)))
    total = reduced[0].astype(F32)
    for i in range(1, copies):
        remote(copy_in.at[i], copy_in.at[i], c_send.at[i], c_recv.at[i], place(d, e, right)).wait_recv()
        total = total + copy_in[i].astype(F32)
    finished[...] = total.astype(BF16)

    @pl.loop(1, n_e)
    def _(i):
        to = (e + i) % n_e
        remote(finished.at[to], back.at[k, s], back_sem.at[0], back_sem.at[1], place(d, to, t)).start()

    back[k, s] = finished[e]
    bulk = arrived.at[0, pl.ds(0, n_e - 1)]
    back_bulk = remote(bulk, bulk, back_sem.at[0], back_sem.at[1], place(d, e, right))
    back_bulk.wait_recv()

    ys, gs = [], []
    for c in range(copies):
        first, second = split_rows(back[:, c].astype(F32))
        ys.append(first.astype(BF16))
        gs.append(second.astype(BF16))
    y, g = jnp.concatenate(ys, axis=1), jnp.concatenate(gs, axis=1)
    chosen0 = jnp.dot(sel0, y, preferred_element_type=F32)
    chosen1 = jnp.dot(sel1, y, preferred_element_type=F32)
    grad_mix = jnp.dot(sel0 + sel1, g, preferred_element_type=F32)
    rows = toks.shape[0]
    diff = jnp.sum(cots * (chosen0 - chosen1), axis=1, keepdims=True)
    dots = jnp.sum(grad_mix * gains * toks, axis=1, keepdims=True)
    column = lax.broadcasted_iota(jnp.int32, (rows, LANES), 1)
    scal_out[...] = jnp.where(column == 0, diff, jnp.where(column == 1, dots, 0.0))
    mixed_all[t] = (toks + (p0 * chosen0 + p1 * chosen1)).astype(BF16)
    for o in range(1, n_t):
        go(remote(scal_out, scal_in.at[o - 1], sc_send.at[o - 1], sc_recv.at[o - 1], place(d, e, (t + o) % n_t)))
    for o in range(1, n_t):
        go(remote(mixed_all.at[t], mixed_all.at[t], mx_send.at[o - 1], mx_recv.at[o - 1],
                  place(d, e, (t + o) % n_t)))
    scalars = scal_out[...]
    for o in range(1, n_t):
        remote(scal_in.at[o - 1], scal_in.at[o - 1], sc_send.at[o - 1], sc_recv.at[o - 1],
               place(d, e, right)).wait_recv()
        scalars = scalars + scal_in[o - 1]
    grad_first = p0 * p1 * scalars[:, 0:1]
    grad_logits = grad_first * sign
    grad_normed = grad_mix
    routers = router_ref[:, sl].astype(F32)
    for j in range(experts):
        grad_normed = grad_normed + grad_logits[:, j : j + 1] * routers[j : j + 1]
    normed32 = normeds.astype(F32)
    router_part = jnp.concatenate(
        [jnp.sum(grad_logits[:, j : j + 1] * normed32, axis=0, keepdims=True) for j in range(experts)], axis=0)
    gain_part = jnp.sum(grad_normed * toks * inv_rms, axis=0, keepdims=True)
    units = sums.shape[1]

    def unit(u):
        return u // units, u % units

    n_half = experts // SLOTS
    for c in range(copies):
        at = slice(c * LANES, (c + 1) * LANES)
        for h in range(n_half):
            a, b = unit(c * n_half + h)
            sums[a, b] = router_part[h * SLOTS : (h + 1) * SLOTS, at]
        a, b = unit(n_half * copies + c // SLOTS)
        sums[a, b, c % SLOTS : c % SLOTS + 1] = gain_part[:, at]

    def member(i):
        j = (line + i) % n_line
        return j, place(j // LINE, z * LINE + j % LINE, t)

    @pl.loop(1, n_line)
    def _(i):
        j, target = member(i)
        remote(sums.at[j], line_in.at[line], line_sem.at[0], line_sem.at[1], target).start()

    mean = (scalars[:, 1:2] + jnp.sum(grad_logits * through, axis=1, keepdims=True)) / (n_t * width)
    cubed = inv_rms * inv_rms * inv_rms
    gtok_all[t] = (cots + inv_rms * (grad_normed * gains) - toks * cubed * mean).astype(BF16)
    for o in range(1, n_t):
        go(remote(gtok_all.at[t], gtok_all.at[t], gt_send.at[o - 1], gt_recv.at[o - 1],
                  place(d, e, (t + o) % n_t)))
    line_in[line] = sums[line]
    some = pl.ds(0, n_line - 1)
    line_bulk = remote(line_in.at[some], line_in.at[some], line_sem.at[0], line_sem.at[1], place(d, e, right))
    line_bulk.wait_recv()
    line_sum[...] = jnp.sum(line_in[...], axis=0)

    if n_z > 1:
        @pl.loop(1, n_z)
        def _(i):
            to = (z + i) % n_z
            remote(line_sum, z_in.at[z], z_sem.at[0], z_sem.at[1], place(d, to * LINE + e % LINE, t)).start()

        z_in[z] = line_sum[...]
        zs = pl.ds(0, n_z - 1)
        z_bulk = remote(z_in.at[zs], z_in.at[zs], z_sem.at[0], z_sem.at[1], place(d, e, right))
        z_bulk.wait_recv()
        z_sum[...] = jnp.sum(z_in[...], axis=0)
    else:
        z_sum[...] = line_sum[...]

    @pl.loop(1, n_line)
    def _(i):
        j, target = member(i)
        remote(z_sum, grads.at[t, line], gl_sem.at[0], gl_sem.at[1], target).start()

    grads[t, line] = z_sum[...]
    gl_bulk = remote(grads.at[t, some], grads.at[t, some], gl_sem.at[0], gl_sem.at[1], place(d, e, right))
    gl_bulk.wait_recv()
    for o in range(1, n_t):
        go(remote(grads.at[t], grads.at[t], gx_send.at[o - 1], gx_recv.at[o - 1], place(d, e, (t + o) % n_t)))

    def other(o):
        return (t + n_t - o) % n_t

    for o in range(1, n_t):
        remote(mixed_all.at[other(o)], mixed_all.at[other(o)], mx_send.at[o - 1], mx_recv.at[o - 1],
               place(d, e, right)).wait_recv()
        remote(gtok_all.at[other(o)], gtok_all.at[other(o)], gt_send.at[o - 1], gt_recv.at[o - 1],
               place(d, e, right)).wait_recv()
    for o in range(1, n_t):
        remote(grads.at[other(o)], grads.at[other(o)], gx_send.at[o - 1], gx_recv.at[o - 1],
               place(d, e, right)).wait_recv()

    a2a.wait_send()
    back_bulk.wait_send()
    line_bulk.wait_send()
    if n_z > 1:
        z_bulk.wait_send()
    gl_bulk.wait_send()
    for copy in started:
        copy.wait_send()


def assemble_kernel(dims, mixed_all, gtok_all, grads, mixed_ref, gtok_ref, grouter_ref, ggain_ref):
    n_dp, n_e, n_t, experts, copies = dims
    width, n_half, units = copies * LANES, experts // SLOTS, grads.shape[2]

    def unit(u):
        return u // units, u % units

    for q in range(n_t):
        at = slice(q * width, (q + 1) * width)
        mixed_ref[:, at] = mixed_all[q]
        gtok_ref[:, at] = gtok_all[q]
        for c in range(copies):
            at = slice(q * width + c * LANES, q * width + (c + 1) * LANES)
            for h in range(n_half):
                a, b = unit(c * n_half + h)
                grouter_ref[h * SLOTS : (h + 1) * SLOTS, at] = grads[q, a, b]
            a, b = unit(n_half * copies + c // SLOTS)
            ggain_ref[:, at] = grads[q, a, b, c % SLOTS : c % SLOTS + 1]


def shards(dims, tokens, cotangent, gain, w_router, w_gate, w_up, w_down, expert_ids, slots):
    n_dp, n_e, n_t, experts, copies = dims
    count, features = tokens.shape
    hidden = w_gate.shape[2]
    width = features // n_t
    n_rows = n_e * SLOTS
    n_line, n_z = n_dp * LINE, n_e // LINE
    units = -(-(copies * (experts // SLOTS) + -(-copies // SLOTS)) // n_line)
    block = (n_e, 8, LANES)
    dma = pltpu.SemaphoreType.DMA
    vmem = pl.BlockSpec(memory_space=pltpu.VMEM)
    scratch = [
        pltpu.VMEM((n_t, width, hidden), BF16), pltpu.VMEM((n_t, width, hidden), BF16),
        pltpu.VMEM((hidden, features), BF16),
        pltpu.VMEM((experts, copies, 8, LANES), BF16),
        pltpu.VMEM((n_t * copies,) + block, BF16),
        pltpu.VMEM((n_rows, width), BF16), pltpu.VMEM((n_rows, width), BF16),
        pltpu.VMEM((3, n_rows, hidden), F32), pltpu.VMEM((3, n_rows, hidden), BF16),
        pltpu.VMEM((n_t, copies) + block, BF16),
        pltpu.VMEM((copies,) + block, BF16), pltpu.VMEM((copies,) + block, BF16),
        pltpu.VMEM((copies,) + block, BF16), pltpu.VMEM((copies,) + block, BF16),
        pltpu.VMEM((copies,) + block, BF16),
        pltpu.VMEM(block, BF16),
        pltpu.VMEM((experts, copies, 8, LANES), BF16),
        pltpu.VMEM((count, LANES), F32), pltpu.VMEM((n_t - 1, count, LANES), F32),
        pltpu.VMEM((n_line, units, SLOTS, LANES), F32), pltpu.VMEM((n_line, units, SLOTS, LANES), F32),
        pltpu.VMEM((units, SLOTS, LANES), F32),
        pltpu.VMEM((n_z, units, SLOTS, LANES), F32), pltpu.VMEM((units, SLOTS, LANES), F32),
        dma((3,)), dma((2,)),
    ] + [dma((copies, BANDS))] * 8 + [dma((copies,))] * 8 + [dma((2,))] + [dma((n_t - 1,))] * 6 + [dma((2,))] * 3 + [dma((n_t - 1,))] * 2
    gathered = pl.pallas_call(
        functools.partial(layer_kernel, dims),
        out_shape=(
            jax.ShapeDtypeStruct((n_t, count, width), BF16), jax.ShapeDtypeStruct((n_t, count, width), BF16),
            jax.ShapeDtypeStruct((n_t, n_line, units, SLOTS, LANES), F32),
        ),
        in_specs=[vmem] * 6 + [pl.BlockSpec(memory_space=pl.ANY)] * 3,
        out_specs=(vmem,) * 3,
        scratch_shapes=scratch,
        compiler_params=pltpu.CompilerParams(
            collective_id=0, has_side_effects=True, vmem_limit_bytes=56 * 1024 * 1024),
    )(
        tokens, cotangent, gain.reshape(1, features), w_router.T, expert_ids.T, slots.T,
        w_gate.reshape(n_t, width, hidden), w_up.reshape(n_t, width, hidden), w_down.reshape(hidden, features),
    )
    mixed, gtok, grouter, ggain = pl.pallas_call(
        functools.partial(assemble_kernel, dims),
        out_shape=(
            jax.ShapeDtypeStruct((count, features), BF16), jax.ShapeDtypeStruct((count, features), BF16),
            jax.ShapeDtypeStruct((experts, features), F32), jax.ShapeDtypeStruct((1, features), F32),
        ),
        in_specs=[vmem] * 3,
        out_specs=(vmem,) * 4,
    )(*gathered)
    return mixed, gtok, grouter.T, ggain.reshape(features)


def solution(mesh):
    n_dp, n_e, n_t = (mesh.shape[a] for a in ("dp", "expert", "tensor"))

    def body(*args):
        experts = args[3].shape[1]
        return shards((n_dp, n_e, n_t, experts, n_e // experts), *args)

    return jax.shard_map(
        body,
        mesh=mesh,
        in_specs=(
            P(("dp", "expert"), None),
            P(("dp", "expert"), None),
            P(),
            P(),
            P("expert", None, "tensor"),
            P("expert", None, "tensor"),
            P("expert", "tensor", None),
            P(("dp", "expert"), None),
            P(("dp", "expert"), None),
        ),
        out_specs=(P(("dp", "expert"), None), P(("dp", "expert"), None), P(), P()),
        check_vma=False,
    )
```

```python
import functools

import jax
import jax.numpy as jnp
from jax import lax
from jax.experimental import pallas as pl
from jax.experimental.pallas import tpu as pltpu
from jax.sharding import PartitionSpec as P

epsilon = 1e-05
LANES = 128
SLOTS = 4
LINE = 4
BANDS = 3
LAG = 3
AHEAD = 2
F32 = jnp.float32
BF16 = jnp.bfloat16
NT = (((1,), (1,)), ((), ()))


def low_rows(shape):
    return lax.broadcasted_iota(jnp.int32, shape, 1) < SLOTS


def split_rows(tiles):
    n = tiles.shape[0]
    pairs = tiles.reshape(n // 2, 2, 8, LANES)
    a, b = pairs[:, 0], pairs[:, 1]
    low = low_rows(a.shape)
    first = jnp.where(low, a, pltpu.roll(b, SLOTS, 1))
    second = jnp.where(low, pltpu.roll(a, SLOTS, 1), b)
    return first.reshape(4 * n, LANES), second.reshape(4 * n, LANES)


def join_rows(first, second):
    n = first.shape[0] // 4
    first = first.reshape(n // 2, 8, LANES)
    second = second.reshape(n // 2, 8, LANES)
    low = low_rows(first.shape)
    a = jnp.where(low, first, pltpu.roll(second, SLOTS, 1))
    b = jnp.where(low, pltpu.roll(first, SLOTS, 1), second)
    return jnp.concatenate([a[:, None], b[:, None]], axis=1).reshape(n, 8, LANES)


def one_hots(ids, slots, experts):
    count, n_rows = ids.shape[1], experts * SLOTS
    rows = ids * SLOTS + slots
    at = lax.broadcasted_iota(jnp.int32, (n_rows, count), 0)
    picks = [(at == rows[c : c + 1]).astype(F32) for c in range(2)]
    expert = lax.broadcasted_iota(jnp.int32, (experts, count), 0)
    signs = (expert == ids[0:1]).astype(F32) - (expert == ids[1:2]).astype(F32)
    both = jnp.concatenate(picks + [signs], axis=0)
    fill = -both.shape[0] % LANES
    both = jnp.concatenate([both, jnp.zeros((fill, count), F32)], axis=0)
    both = jnp.concatenate([both, jnp.zeros((both.shape[0], LANES - count), F32)], axis=1)
    turned = both.T
    sel0 = turned[:count, :n_rows].astype(BF16)
    sel1 = turned[:count, n_rows : 2 * n_rows].astype(BF16)
    sign = turned[:count, 2 * n_rows : 2 * n_rows + experts]
    return sel0, sel1, sign, picks[0].astype(BF16), picks[1].astype(BF16)


def swapped(k, s, copies):
    if copies != 6:
        return s
    a = 1 + 2 * modulo(k, 2)

    def equal(n):
        return divide(copies - modulo(s - n + copies, copies), copies)

    return s + equal(a) - equal(a + 1)


def far_first(n):
    return sorted(range(1, n), key=lambda i: -min(i, n - i))


def divide(a, n):
    return lax.div(a, jnp.int32(n))


def modulo(a, n):
    return lax.rem(a, jnp.int32(n))


def layer_kernel(
    dims,
    tokens_ref, cot_ref, gain_ref, router_ref, ids_ref, slots_ref,
    gate_hbm, up_hbm, down_hbm,
    mixed_all, gtok_all, grads,
    wg, wu, wd, packed, arrived, xin, gin, pre, hid, parts, fwd_in, left_in, right_in, reduced,
    copy_in, finished, back, scal_out, scal_in, sums, line_in, line_sum, z_in, z_sum,
    w_sem, a2a_sem, cp_send, cp_recv, xl_send, xr_send, xf_send, xl_recv, xr_recv, xf_recv,
    f_send, f_recv, l_send, r_send, l_recv, r_recv, c_send, c_recv, back_sem,
    sc_send, sc_recv, mx_send, mx_recv, gt_send, gt_recv, line_sem, z_sem, gl_sem, gx_send, gx_recv,
):
    n_dp, n_e, n_t, experts, copies = dims
    width = copies * LANES
    half = copies // 2
    d, e, t = lax.axis_index("dp"), lax.axis_index("expert"), lax.axis_index("tensor")
    k = e // copies
    p = swapped(k, e % copies, copies)
    pair = p // 2 * 2
    z, line = e // LINE, d * LINE + e % LINE
    n_z, n_line = n_e // LINE, n_dp * LINE
    left, right, across = (t + n_t - 1) % n_t, (t + 1) % n_t, (t + 2) % n_t
    mine = pl.ds(t * copies + pair, 2)
    sl = pl.ds(pl.multiple_of(t * width, LANES), width)

    def place(dp, expert, tensor):
        return (dp, expert, tensor)

    def remote(src, dst, send, recv, target):
        return pltpu.make_async_remote_copy(
            src_ref=src, dst_ref=dst, send_sem=send, recv_sem=recv,
            device_id=target, device_id_type=pl.DeviceIdType.MESH,
        )

    weights = [
        pltpu.make_async_copy(a, b, w_sem.at[i])
        for i, (a, b) in enumerate(((gate_hbm, wg), (up_hbm, wu), (down_hbm, wd)))
    ]
    for w in weights:
        w.start()

    rows_of = [modulo(modulo(e, LINE) + dy, LINE) for dy in range(LINE)]
    plane_of = [modulo(z + dz, n_z) * LINE for dz in range(n_z)]

    def to_everyone(send):
        near = far_first(LINE)

        @pl.loop(1, n_z)
        def _(i):
            dz = divide(i, 2) * (1 - 2 * modulo(i, 2)) + n_z // 2
            base = modulo(z + dz + n_z, n_z) * LINE
            for dy in near + [0]:
                send(base + rows_of[dy])

        for dy in near:
            send(z * LINE + rows_of[dy])

    bar = pltpu.get_barrier_semaphore()

    to_everyone(lambda to: pl.semaphore_signal(
        bar, inc=1, device_id=place(d, to, t), device_id_type=pl.DeviceIdType.MESH))

    for o in range(1, n_t):
        pl.semaphore_signal(bar, inc=1, device_id=place(d, e, (t + o) % n_t),
                            device_id_type=pl.DeviceIdType.MESH)

    @pl.loop(0, (n_dp - 1) * LINE)
    def _(i):
        pl.semaphore_signal(
            bar, inc=1, device_id=place((d + 1 + i // LINE) % n_dp, z * LINE + i % LINE, t),
            device_id_type=pl.DeviceIdType.MESH)

    floats = tokens_ref[...].astype(F32)
    inv_rms = lax.rsqrt(jnp.mean(floats * floats, axis=1, keepdims=True) + epsilon)
    normed = (floats * inv_rms * gain_ref[...]).astype(BF16)
    logits = lax.dot_general(normed, router_ref[...], NT, preferred_element_type=F32)
    sel0, sel1, sign, selT0, selT1 = one_hots(ids_ref[...], slots_ref[...], experts)
    p0 = jax.nn.sigmoid(jnp.sum(logits * sign, axis=1, keepdims=True))
    p1 = 1.0 - p0
    toks = tokens_ref[:, sl].astype(F32)
    cots = cot_ref[:, sl].astype(F32)
    gains = gain_ref[:, sl]
    normeds = (toks * inv_rms * gains).astype(BF16)
    rows_in = jnp.dot(selT0 + selT1, normeds, preferred_element_type=F32)
    rows_g = (jnp.dot(selT0, (p0 * cots).astype(BF16), preferred_element_type=F32)
              + jnp.dot(selT1, (p1 * cots).astype(BF16), preferred_element_type=F32))
    for c in range(copies):
        at = slice(c * LANES, (c + 1) * LANES)
        packed[:, c] = join_rows(rows_in[:, at], rows_g[:, at]).astype(BF16)

    pl.semaphore_wait(bar, n_e - 1 + n_t - 1 + (n_dp - 1) * LINE)

    def hand_out(to):
        expert = divide(to, copies)
        both = divide(swapped(expert, to - expert * copies, copies), 2) * 2
        remote(packed.at[expert, pl.ds(both, 2)], arrived.at[pl.ds(t * copies + both, 2), e],
               a2a_sem.at[0], a2a_sem.at[1], place(d, to, t)).start()

    to_everyone(hand_out)

    for i in range(2):
        arrived[t * copies + pair + i, e] = packed[k, pair + i]
    scaled = floats * gain_ref[...]
    router = router_ref[...].astype(F32)
    through = jnp.concatenate(
        [jnp.sum(scaled * router[j : j + 1], axis=1, keepdims=True) for j in range(experts)], axis=1)

    a2a = remote(arrived.at[mine, pl.ds(0, n_e - 1)], arrived.at[mine, pl.ds(0, n_e - 1)],
                 a2a_sem.at[0], a2a_sem.at[1], place(d, e, right))
    a2a.wait_recv()

    def piece(i):
        return (pair + i) % copies

    def holder(q):
        return k * copies + swapped(k, q, copies)

    started = []

    def go(copy):
        copy.start()
        started.append(copy)

    bands = cp_send.shape[1]
    span = n_e // bands

    def band(tensor, i, h):
        return arrived.at[tensor * copies + piece(i), pl.ds(h * span, span)]

    def arrives(block, recv):
        remote(block, block, cp_send.at[0, 0], recv, place(d, e, right)).wait_recv()

    def to_copies(h):
        for i in range(2, copies):
            to = (pair + (copies - 2 if i < 4 else 2) + i % 2) % copies
            own = arrived.at[t * copies + p, pl.ds(h * span, span)]
            go(remote(own, own, cp_send.at[i, h], cp_recv.at[p, h], place(d, holder(to), t)))

    to_copies(0)

    def both_ways(i, h):
        block = band(t, i, h)
        go(remote(block, block, xr_send.at[i, h], xr_recv.at[i, h], place(d, e, right)))
        go(remote(block, block, xl_send.at[i, h], xl_recv.at[i, h], place(d, e, left)))

    def pass_on(i, h):
        arrives(band(left, i, h), xr_recv.at[i, h])
        arrives(band(right, i, h), xl_recv.at[i, h])
        block, to = (band(left, i, h), right) if i < half else (band(right, i, h), left)
        go(remote(block, block, xf_send.at[i, h], xf_recv.at[i, h], place(d, e, to)))

    steps = ([(i, h) for h in range(bands) for i in range(2)]
             + [(i, h) for h in range(bands) for i in range(2, copies)])
    waiting = []
    for i, h in steps:
        if i > 1:
            arrives(band(t, i, h), cp_recv.at[piece(i), h])
        both_ways(i, h)
        if i == AHEAD and h + 1 < bands:
            to_copies(h + 1)
        waiting.append((i, h))
        if len(waiting) > LAG:
            pass_on(*waiting.pop(0))
    for i, h in waiting:
        pass_on(i, h)

    pre[...] = jnp.zeros_like(pre)
    for w in weights:
        w.wait()

    def features(q):
        for c in range(copies):
            first, second = split_rows(arrived[q * copies + c].astype(F32))
            at = slice(c * LANES, (c + 1) * LANES)
            xin[:, at] = first.astype(BF16)
            gin[:, at] = second.astype(BF16)
        x, g = xin[...], gin[...]
        pre[0] += jnp.dot(x, wg[q], preferred_element_type=F32)
        pre[1] += jnp.dot(x, wu[q], preferred_element_type=F32)
        down = wd[:, pl.ds(pl.multiple_of(q * width, LANES), width)]
        pre[2] += lax.dot_general(g, down, NT, preferred_element_type=F32)

    @pl.loop(0, n_t - 1)
    def _(j):
        features((t + jnp.where(j == 2, 3, j)) % n_t)

    for i, h in steps:
        arrives(band(across, i, h), xf_recv.at[i, h])
    features(across)

    gate, up, grad_act = pre[0], pre[1], pre[2]
    sig = jax.nn.sigmoid(gate)
    silu = gate * sig
    hid[0] = (silu * up).astype(BF16)
    hid[1] = (grad_act * up * sig * (1.0 + gate * (1.0 - sig))).astype(BF16)
    hid[2] = (grad_act * silu).astype(BF16)

    def quarter(q):
        down = wd[:, pl.ds(pl.multiple_of(q * width, LANES), width)]
        y = jnp.dot(hid[0], down, preferred_element_type=F32)
        g = (lax.dot_general(hid[1], wg[q], NT, preferred_element_type=F32)
             + lax.dot_general(hid[2], wu[q], NT, preferred_element_type=F32))
        for c in range(copies):
            at = slice(c * LANES, (c + 1) * LANES)
            parts[q, c] = join_rows(y[:, at], g[:, at]).astype(BF16)

    order = [(i + 1) % copies for i in range(copies)]

    def piece(i):
        return (p + i) % copies

    quarter(across)
    for i in order:
        src = parts.at[across, piece(i)]
        go(remote(src, fwd_in.at[i], f_send.at[i], f_recv.at[i], place(d, e, right if i < half else left)))

    @pl.loop(0, 3)
    def _(j):
        quarter((t + jnp.where(j == 0, 1, jnp.where(j == 1, n_t - 1, 0))) % n_t)

    for i in order:
        remote(fwd_in.at[i], fwd_in.at[i], f_send.at[i], f_recv.at[i], place(d, e, right)).wait_recv()
        on = right if i < half else left
        parts[on, piece(i)] = (parts[on, piece(i)].astype(F32) + fwd_in[i].astype(F32)).astype(BF16)
        go(remote(parts.at[right, piece(i)], left_in.at[i], r_send.at[i], r_recv.at[i], place(d, e, right)))
        go(remote(parts.at[left, piece(i)], right_in.at[i], l_send.at[i], l_recv.at[i], place(d, e, left)))

    for i in order:
        remote(left_in.at[i], left_in.at[i], r_send.at[i], r_recv.at[i], place(d, e, right)).wait_recv()
        remote(right_in.at[i], right_in.at[i], l_send.at[i], l_recv.at[i], place(d, e, left)).wait_recv()
        total = parts[t, piece(i)].astype(F32) + left_in[i].astype(F32) + right_in[i].astype(F32)
        reduced[i] = total.astype(BF16)
        if i > 0:
            go(remote(reduced.at[i], copy_in.at[i], c_send.at[i], c_recv.at[i],
                      place(d, holder(piece(i)), t)))
    total = reduced[0].astype(F32)
    for i in range(1, copies):
        remote(copy_in.at[i], copy_in.at[i], c_send.at[i], c_recv.at[i], place(d, e, right)).wait_recv()
        total = total + copy_in[i].astype(F32)
    finished[...] = total.astype(BF16)

    to_everyone(lambda to: remote(
        finished.at[to], back.at[k, p], back_sem.at[0], back_sem.at[1], place(d, to, t)).start())

    back[k, p] = finished[e]
    bulk = arrived.at[0, pl.ds(0, n_e - 1)]
    back_bulk = remote(bulk, bulk, back_sem.at[0], back_sem.at[1], place(d, e, right))
    back_bulk.wait_recv()

    ys, gs = [], []
    for c in range(copies):
        first, second = split_rows(back[:, c].astype(F32))
        ys.append(first.astype(BF16))
        gs.append(second.astype(BF16))
    y, g = jnp.concatenate(ys, axis=1), jnp.concatenate(gs, axis=1)
    chosen0 = jnp.dot(sel0, y, preferred_element_type=F32)
    chosen1 = jnp.dot(sel1, y, preferred_element_type=F32)
    grad_mix = jnp.dot(sel0 + sel1, g, preferred_element_type=F32)
    rows = toks.shape[0]
    diff = jnp.sum(cots * (chosen0 - chosen1), axis=1, keepdims=True)
    dots = jnp.sum(grad_mix * gains * toks, axis=1, keepdims=True)
    column = lax.broadcasted_iota(jnp.int32, (rows, LANES), 1)
    scal_out[...] = jnp.where(column == 0, diff, jnp.where(column == 1, dots, 0.0))
    mixed_all[t] = (toks + (p0 * chosen0 + p1 * chosen1)).astype(BF16)
    for o in range(1, n_t):
        go(remote(scal_out, scal_in.at[o - 1], sc_send.at[o - 1], sc_recv.at[o - 1], place(d, e, (t + o) % n_t)))
    for o in range(1, n_t):
        go(remote(mixed_all.at[t], mixed_all.at[t], mx_send.at[o - 1], mx_recv.at[o - 1],
                  place(d, e, (t + o) % n_t)))
    scalars = scal_out[...]
    for o in range(1, n_t):
        remote(scal_in.at[o - 1], scal_in.at[o - 1], sc_send.at[o - 1], sc_recv.at[o - 1],
               place(d, e, right)).wait_recv()
        scalars = scalars + scal_in[o - 1]
    grad_first = p0 * p1 * scalars[:, 0:1]
    grad_logits = grad_first * sign
    grad_normed = grad_mix
    routers = router_ref[:, sl].astype(F32)
    for j in range(experts):
        grad_normed = grad_normed + grad_logits[:, j : j + 1] * routers[j : j + 1]
    normed32 = normeds.astype(F32)
    router_part = jnp.concatenate(
        [jnp.sum(grad_logits[:, j : j + 1] * normed32, axis=0, keepdims=True) for j in range(experts)], axis=0)
    gain_part = jnp.sum(grad_normed * toks * inv_rms, axis=0, keepdims=True)
    units = sums.shape[1]

    def unit(u):
        return u // units, u % units

    n_half = experts // SLOTS
    for c in range(copies):
        at = slice(c * LANES, (c + 1) * LANES)
        for h in range(n_half):
            a, b = unit(c * n_half + h)
            sums[a, b] = router_part[h * SLOTS : (h + 1) * SLOTS, at]
        a, b = unit(n_half * copies + c // SLOTS)
        sums[a, b, c % SLOTS : c % SLOTS + 1] = gain_part[:, at]

    near = far_first(LINE) + [0]
    members = []
    for dy in near:
        for dd in range(n_dp):
            if dy or dd:
                there = modulo(d + dd, n_dp)
                members.append((there * LINE + rows_of[dy], place(there, z * LINE + rows_of[dy], t)))

    for j, target in members:
        remote(sums.at[j], line_in.at[line], line_sem.at[0], line_sem.at[1], target).start()

    mean = (scalars[:, 1:2] + jnp.sum(grad_logits * through, axis=1, keepdims=True)) / (n_t * width)
    cubed = inv_rms * inv_rms * inv_rms
    gtok_all[t] = (cots + inv_rms * (grad_normed * gains) - toks * cubed * mean).astype(BF16)
    for o in range(1, n_t):
        go(remote(gtok_all.at[t], gtok_all.at[t], gt_send.at[o - 1], gt_recv.at[o - 1],
                  place(d, e, (t + o) % n_t)))
    line_in[line] = sums[line]
    some = pl.ds(0, n_line - 1)
    line_bulk = remote(line_in.at[some], line_in.at[some], line_sem.at[0], line_sem.at[1], place(d, e, right))
    line_bulk.wait_recv()
    line_sum[...] = jnp.sum(line_in[...], axis=0)

    if n_z > 1:
        for dz in far_first(n_z):
            remote(line_sum, z_in.at[z], z_sem.at[0], z_sem.at[1], place(d, plane_of[dz] + rows_of[0], t)).start()

        z_in[z] = line_sum[...]
        zs = pl.ds(0, n_z - 1)
        z_bulk = remote(z_in.at[zs], z_in.at[zs], z_sem.at[0], z_sem.at[1], place(d, e, right))
        z_bulk.wait_recv()
        z_sum[...] = jnp.sum(z_in[...], axis=0)
    else:
        z_sum[...] = line_sum[...]

    for j, target in members:
        remote(z_sum, grads.at[t, line], gl_sem.at[0], gl_sem.at[1], target).start()

    grads[t, line] = z_sum[...]
    gl_bulk = remote(grads.at[t, some], grads.at[t, some], gl_sem.at[0], gl_sem.at[1], place(d, e, right))
    gl_bulk.wait_recv()
    for o in range(1, n_t):
        go(remote(grads.at[t], grads.at[t], gx_send.at[o - 1], gx_recv.at[o - 1], place(d, e, (t + o) % n_t)))

    def other(o):
        return (t + n_t - o) % n_t

    for o in range(1, n_t):
        remote(mixed_all.at[other(o)], mixed_all.at[other(o)], mx_send.at[o - 1], mx_recv.at[o - 1],
               place(d, e, right)).wait_recv()
        remote(gtok_all.at[other(o)], gtok_all.at[other(o)], gt_send.at[o - 1], gt_recv.at[o - 1],
               place(d, e, right)).wait_recv()
    for o in range(1, n_t):
        remote(grads.at[other(o)], grads.at[other(o)], gx_send.at[o - 1], gx_recv.at[o - 1],
               place(d, e, right)).wait_recv()

    a2a.wait_send()
    back_bulk.wait_send()
    line_bulk.wait_send()
    if n_z > 1:
        z_bulk.wait_send()
    gl_bulk.wait_send()
    for copy in started:
        copy.wait_send()


def assemble_kernel(dims, mixed_all, gtok_all, grads, mixed_ref, gtok_ref, grouter_ref, ggain_ref):
    n_dp, n_e, n_t, experts, copies = dims
    width, n_half, units = copies * LANES, experts // SLOTS, grads.shape[2]

    def unit(u):
        return u // units, u % units

    for q in range(n_t):
        at = slice(q * width, (q + 1) * width)
        mixed_ref[:, at] = mixed_all[q]
        gtok_ref[:, at] = gtok_all[q]
        for c in range(copies):
            at = slice(q * width + c * LANES, q * width + (c + 1) * LANES)
            for h in range(n_half):
                a, b = unit(c * n_half + h)
                grouter_ref[h * SLOTS : (h + 1) * SLOTS, at] = grads[q, a, b]
            a, b = unit(n_half * copies + c // SLOTS)
            ggain_ref[:, at] = grads[q, a, b, c % SLOTS : c % SLOTS + 1]


def shards(dims, tokens, cotangent, gain, w_router, w_gate, w_up, w_down, expert_ids, slots):
    n_dp, n_e, n_t, experts, copies = dims
    count, features = tokens.shape
    hidden = w_gate.shape[2]
    width = features // n_t
    n_rows = n_e * SLOTS
    n_line, n_z = n_dp * LINE, n_e // LINE
    units = -(-(copies * (experts // SLOTS) + -(-copies // SLOTS)) // n_line)
    block = (n_e, 8, LANES)
    dma = pltpu.SemaphoreType.DMA
    vmem = pl.BlockSpec(memory_space=pltpu.VMEM)
    scratch = [
        pltpu.VMEM((n_t, width, hidden), BF16), pltpu.VMEM((n_t, width, hidden), BF16),
        pltpu.VMEM((hidden, features), BF16),
        pltpu.VMEM((experts, copies, 8, LANES), BF16),
        pltpu.VMEM((n_t * copies,) + block, BF16),
        pltpu.VMEM((n_rows, width), BF16), pltpu.VMEM((n_rows, width), BF16),
        pltpu.VMEM((3, n_rows, hidden), F32), pltpu.VMEM((3, n_rows, hidden), BF16),
        pltpu.VMEM((n_t, copies) + block, BF16),
        pltpu.VMEM((copies,) + block, BF16), pltpu.VMEM((copies,) + block, BF16),
        pltpu.VMEM((copies,) + block, BF16), pltpu.VMEM((copies,) + block, BF16),
        pltpu.VMEM((copies,) + block, BF16),
        pltpu.VMEM(block, BF16),
        pltpu.VMEM((experts, copies, 8, LANES), BF16),
        pltpu.VMEM((count, LANES), F32), pltpu.VMEM((n_t - 1, count, LANES), F32),
        pltpu.VMEM((n_line, units, SLOTS, LANES), F32), pltpu.VMEM((n_line, units, SLOTS, LANES), F32),
        pltpu.VMEM((units, SLOTS, LANES), F32),
        pltpu.VMEM((n_z, units, SLOTS, LANES), F32), pltpu.VMEM((units, SLOTS, LANES), F32),
        dma((3,)), dma((2,)),
    ] + [dma((copies, BANDS))] * 8 + [dma((copies,))] * 8 + [dma((2,))] + [dma((n_t - 1,))] * 6 + [dma((2,))] * 3 + [dma((n_t - 1,))] * 2
    gathered = pl.pallas_call(
        functools.partial(layer_kernel, dims),
        out_shape=(
            jax.ShapeDtypeStruct((n_t, count, width), BF16), jax.ShapeDtypeStruct((n_t, count, width), BF16),
            jax.ShapeDtypeStruct((n_t, n_line, units, SLOTS, LANES), F32),
        ),
        in_specs=[vmem] * 6 + [pl.BlockSpec(memory_space=pl.ANY)] * 3,
        out_specs=(vmem,) * 3,
        scratch_shapes=scratch,
        compiler_params=pltpu.CompilerParams(
            collective_id=0, has_side_effects=True, vmem_limit_bytes=56 * 1024 * 1024),
    )(
        tokens, cotangent, gain.reshape(1, features), w_router.T, expert_ids.T, slots.T,
        w_gate.reshape(n_t, width, hidden), w_up.reshape(n_t, width, hidden), w_down.reshape(hidden, features),
    )
    mixed, gtok, grouter, ggain = pl.pallas_call(
        functools.partial(assemble_kernel, dims),
        out_shape=(
            jax.ShapeDtypeStruct((count, features), BF16), jax.ShapeDtypeStruct((count, features), BF16),
            jax.ShapeDtypeStruct((experts, features), F32), jax.ShapeDtypeStruct((1, features), F32),
        ),
        in_specs=[vmem] * 3,
        out_specs=(vmem,) * 4,
    )(*gathered)
    return mixed, gtok, grouter.T, ggain.reshape(features)


def solution(mesh):
    n_dp, n_e, n_t = (mesh.shape[a] for a in ("dp", "expert", "tensor"))

    def body(*args):
        experts = args[3].shape[1]
        return shards((n_dp, n_e, n_t, experts, n_e // experts), *args)

    return jax.shard_map(
        body,
        mesh=mesh,
        in_specs=(
            P(("dp", "expert"), None),
            P(("dp", "expert"), None),
            P(),
            P(),
            P("expert", None, "tensor"),
            P("expert", None, "tensor"),
            P("expert", "tensor", None),
            P(("dp", "expert"), None),
            P(("dp", "expert"), None),
        ),
        out_specs=(P(("dp", "expert"), None), P(("dp", "expert"), None), P(), P()),
        check_vma=False,
    )
```

```python
import functools

import jax
import jax.numpy as jnp
from jax import lax
from jax.experimental import pallas as pl
from jax.experimental.pallas import tpu as pltpu
from jax.sharding import PartitionSpec as P

epsilon = 1e-05
LANES = 128
SLOTS = 4
LINE = 4
BANDS = 3
LAG = 7
AHEAD = 2
F32 = jnp.float32
BF16 = jnp.bfloat16
NT = (((1,), (1,)), ((), ()))


def low_rows(shape):
    return lax.broadcasted_iota(jnp.int32, shape, 1) < SLOTS


def split_rows(tiles):
    n = tiles.shape[0]
    pairs = tiles.reshape(n // 2, 2, 8, LANES)
    a, b = pairs[:, 0], pairs[:, 1]
    low = low_rows(a.shape)
    first = jnp.where(low, a, pltpu.roll(b, SLOTS, 1))
    second = jnp.where(low, pltpu.roll(a, SLOTS, 1), b)
    return first.reshape(4 * n, LANES), second.reshape(4 * n, LANES)


def join_rows(first, second):
    n = first.shape[0] // 4
    first = first.reshape(n // 2, 8, LANES)
    second = second.reshape(n // 2, 8, LANES)
    low = low_rows(first.shape)
    a = jnp.where(low, first, pltpu.roll(second, SLOTS, 1))
    b = jnp.where(low, pltpu.roll(first, SLOTS, 1), second)
    return jnp.concatenate([a[:, None], b[:, None]], axis=1).reshape(n, 8, LANES)


def one_hots(ids, slots, experts):
    count, n_rows = ids.shape[1], experts * SLOTS
    rows = ids * SLOTS + slots
    at = lax.broadcasted_iota(jnp.int32, (n_rows, count), 0)
    picks = [(at == rows[c : c + 1]).astype(F32) for c in range(2)]
    expert = lax.broadcasted_iota(jnp.int32, (experts, count), 0)
    signs = (expert == ids[0:1]).astype(F32) - (expert == ids[1:2]).astype(F32)
    both = jnp.concatenate(picks + [signs], axis=0)
    fill = -both.shape[0] % LANES
    both = jnp.concatenate([both, jnp.zeros((fill, count), F32)], axis=0)
    both = jnp.concatenate([both, jnp.zeros((both.shape[0], LANES - count), F32)], axis=1)
    turned = both.T
    sel0 = turned[:count, :n_rows].astype(BF16)
    sel1 = turned[:count, n_rows : 2 * n_rows].astype(BF16)
    sign = turned[:count, 2 * n_rows : 2 * n_rows + experts]
    return sel0, sel1, sign, picks[0].astype(BF16), picks[1].astype(BF16)


def swapped(k, s, copies):
    if copies != 6:
        return s
    a = 1 + 2 * modulo(k, 2)

    def equal(n):
        return divide(copies - modulo(s - n + copies, copies), copies)

    return s + equal(a) - equal(a + 1)


def far_first(n):
    return sorted(range(1, n), key=lambda i: -min(i, n - i))


def divide(a, n):
    return lax.div(a, jnp.int32(n))


def modulo(a, n):
    return lax.rem(a, jnp.int32(n))


def layer_kernel(
    dims,
    tokens_ref, cot_ref, gain_ref, router_ref, ids_ref, slots_ref,
    gate_hbm, up_hbm, down_hbm,
    mixed_all, gtok_all, grads,
    wg, wu, wd, packed, arrived, xin, gin, pre, hid, parts, fwd_in, left_in, right_in, reduced,
    copy_in, finished, back, scal_out, scal_in, sums, line_in, line_sum, z_in, z_sum,
    w_sem, a2a_sem, cp_send, cp_recv, xl_send, xr_send, xf_send, xl_recv, xr_recv, xf_recv,
    f_send, f_recv, l_send, r_send, l_recv, r_recv, c_send, c_recv, back_sem,
    sc_send, sc_recv, mx_send, mx_recv, gt_send, gt_recv, line_sem, z_sem, gl_sem, gx_send, gx_recv,
):
    n_dp, n_e, n_t, experts, copies = dims
    width = copies * LANES
    half = copies // 2
    d, e, t = lax.axis_index("dp"), lax.axis_index("expert"), lax.axis_index("tensor")
    k = e // copies
    p = swapped(k, e % copies, copies)
    pair = p // 2 * 2
    z, line = e // LINE, d * LINE + e % LINE
    n_z, n_line = n_e // LINE, n_dp * LINE
    left, right, across = (t + n_t - 1) % n_t, (t + 1) % n_t, (t + 2) % n_t
    mine = pl.ds(t * copies + pair, 2)
    sl = pl.ds(pl.multiple_of(t * width, LANES), width)

    def place(dp, expert, tensor):
        return (dp, expert, tensor)

    def remote(src, dst, send, recv, target):
        return pltpu.make_async_remote_copy(
            src_ref=src, dst_ref=dst, send_sem=send, recv_sem=recv,
            device_id=target, device_id_type=pl.DeviceIdType.MESH,
        )

    weights = [
        pltpu.make_async_copy(a, b, w_sem.at[i])
        for i, (a, b) in enumerate(((gate_hbm, wg), (up_hbm, wu), (down_hbm, wd)))
    ]
    for w in weights:
        w.start()

    rows_of = [modulo(modulo(e, LINE) + dy, LINE) for dy in range(LINE)]
    plane_of = [modulo(z + dz, n_z) * LINE for dz in range(n_z)]

    def to_everyone(send):
        near = far_first(LINE)

        @pl.loop(1, n_z)
        def _(i):
            dz = divide(i, 2) * (1 - 2 * modulo(i, 2)) + n_z // 2
            base = modulo(z + dz + n_z, n_z) * LINE
            for dy in near + [0]:
                send(base + rows_of[dy])

        for dy in near:
            send(z * LINE + rows_of[dy])

    bar = pltpu.get_barrier_semaphore()

    to_everyone(lambda to: pl.semaphore_signal(
        bar, inc=1, device_id=place(d, to, t), device_id_type=pl.DeviceIdType.MESH))

    for o in range(1, n_t):
        pl.semaphore_signal(bar, inc=1, device_id=place(d, e, (t + o) % n_t),
                            device_id_type=pl.DeviceIdType.MESH)

    @pl.loop(0, (n_dp - 1) * LINE)
    def _(i):
        pl.semaphore_signal(
            bar, inc=1, device_id=place((d + 1 + i // LINE) % n_dp, z * LINE + i % LINE, t),
            device_id_type=pl.DeviceIdType.MESH)

    floats = tokens_ref[...].astype(F32)
    inv_rms = lax.rsqrt(jnp.mean(floats * floats, axis=1, keepdims=True) + epsilon)
    normed = (floats * inv_rms * gain_ref[...]).astype(BF16)
    logits = lax.dot_general(normed, router_ref[...], NT, preferred_element_type=F32)
    sel0, sel1, sign, selT0, selT1 = one_hots(ids_ref[...], slots_ref[...], experts)
    p0 = jax.nn.sigmoid(jnp.sum(logits * sign, axis=1, keepdims=True))
    p1 = 1.0 - p0
    toks = tokens_ref[:, sl].astype(F32)
    cots = cot_ref[:, sl].astype(F32)
    gains = gain_ref[:, sl]
    normeds = (toks * inv_rms * gains).astype(BF16)
    rows_in = jnp.dot(selT0 + selT1, normeds, preferred_element_type=F32)
    rows_g = (jnp.dot(selT0, (p0 * cots).astype(BF16), preferred_element_type=F32)
              + jnp.dot(selT1, (p1 * cots).astype(BF16), preferred_element_type=F32))
    for c in range(copies):
        at = slice(c * LANES, (c + 1) * LANES)
        packed[:, c] = join_rows(rows_in[:, at], rows_g[:, at]).astype(BF16)

    pl.semaphore_wait(bar, n_e - 1 + n_t - 1 + (n_dp - 1) * LINE)

    def hand_out(to):
        expert = divide(to, copies)
        both = divide(swapped(expert, to - expert * copies, copies), 2) * 2
        remote(packed.at[expert, pl.ds(both, 2)], arrived.at[pl.ds(t * copies + both, 2), e],
               a2a_sem.at[0], a2a_sem.at[1], place(d, to, t)).start()

    to_everyone(hand_out)

    for i in range(2):
        arrived[t * copies + pair + i, e] = packed[k, pair + i]
    scaled = floats * gain_ref[...]
    router = router_ref[...].astype(F32)
    through = jnp.concatenate(
        [jnp.sum(scaled * router[j : j + 1], axis=1, keepdims=True) for j in range(experts)], axis=1)

    a2a = remote(arrived.at[mine, pl.ds(0, n_e - 1)], arrived.at[mine, pl.ds(0, n_e - 1)],
                 a2a_sem.at[0], a2a_sem.at[1], place(d, e, right))
    a2a.wait_recv()

    def piece(i):
        return (pair + i) % copies

    def holder(q):
        return k * copies + swapped(k, q, copies)

    started = []

    def go(copy):
        copy.start()
        started.append(copy)

    bands = cp_send.shape[1]
    span = n_e // bands

    def band(tensor, i, h):
        return arrived.at[tensor * copies + piece(i), pl.ds(h * span, span)]

    def arrives(block, recv):
        remote(block, block, cp_send.at[0, 0], recv, place(d, e, right)).wait_recv()

    def to_copies(h):
        for i in range(2, copies):
            to = (pair + (copies - 2 if i < 4 else 2) + i % 2) % copies
            own = arrived.at[t * copies + p, pl.ds(h * span, span)]
            go(remote(own, own, cp_send.at[i, h], cp_recv.at[p, h], place(d, holder(to), t)))

    to_copies(0)

    def both_ways(i, h):
        block = band(t, i, h)
        go(remote(block, block, xr_send.at[i, h], xr_recv.at[i, h], place(d, e, right)))
        go(remote(block, block, xl_send.at[i, h], xl_recv.at[i, h], place(d, e, left)))

    def pass_on(i, h):
        arrives(band(left, i, h), xr_recv.at[i, h])
        arrives(band(right, i, h), xl_recv.at[i, h])
        block, to = (band(left, i, h), right) if i < half else (band(right, i, h), left)
        go(remote(block, block, xf_send.at[i, h], xf_recv.at[i, h], place(d, e, to)))

    steps = ([(i, h) for h in range(bands) for i in range(2)]
             + [(i, h) for h in range(bands) for i in range(2, copies)])
    waiting = []
    for i, h in steps:
        if i > 1:
            arrives(band(t, i, h), cp_recv.at[piece(i), h])
        both_ways(i, h)
        if i == AHEAD and h + 1 < bands:
            to_copies(h + 1)
        waiting.append((i, h))
        if len(waiting) > LAG:
            pass_on(*waiting.pop(0))
    pre[...] = jnp.zeros_like(pre)
    for w in weights:
        w.wait()

    def features(q):
        for c in range(copies):
            first, second = split_rows(arrived[q * copies + c].astype(F32))
            at = slice(c * LANES, (c + 1) * LANES)
            xin[:, at] = first.astype(BF16)
            gin[:, at] = second.astype(BF16)
        x, g = xin[...], gin[...]
        pre[0] += jnp.dot(x, wg[q], preferred_element_type=F32)
        pre[1] += jnp.dot(x, wu[q], preferred_element_type=F32)
        down = wd[:, pl.ds(pl.multiple_of(q * width, LANES), width)]
        pre[2] += lax.dot_general(g, down, NT, preferred_element_type=F32)

    features(t)
    for i, h in waiting:
        pass_on(i, h)

    @pl.loop(0, 2)
    def _(j):
        features((t + 1 + 2 * j) % n_t)

    for i, h in steps:
        arrives(band(across, i, h), xf_recv.at[i, h])
    features(across)

    gate, up, grad_act = pre[0], pre[1], pre[2]
    sig = jax.nn.sigmoid(gate)
    silu = gate * sig
    hid[0] = (silu * up).astype(BF16)
    hid[1] = (grad_act * up * sig * (1.0 + gate * (1.0 - sig))).astype(BF16)
    hid[2] = (grad_act * silu).astype(BF16)

    def quarter(q):
        down = wd[:, pl.ds(pl.multiple_of(q * width, LANES), width)]
        y = jnp.dot(hid[0], down, preferred_element_type=F32)
        g = (lax.dot_general(hid[1], wg[q], NT, preferred_element_type=F32)
             + lax.dot_general(hid[2], wu[q], NT, preferred_element_type=F32))
        for c in range(copies):
            at = slice(c * LANES, (c + 1) * LANES)
            parts[q, c] = join_rows(y[:, at], g[:, at]).astype(BF16)

    order = [i for pair_of in zip(range(1, half), range(half, copies)) for i in pair_of] + [copies - 1, 0]

    def piece(i):
        return (p + i) % copies

    quarter(across)
    for i in order:
        src = parts.at[across, piece(i)]
        go(remote(src, fwd_in.at[i], f_send.at[i], f_recv.at[i], place(d, e, right if i < half else left)))

    @pl.loop(0, 2)
    def _(j):
        quarter((t + 1 + 2 * j) % n_t)

    def to_right(i):
        go(remote(parts.at[right, piece(i)], left_in.at[i], r_send.at[i], r_recv.at[i], place(d, e, right)))

    def to_left(i):
        go(remote(parts.at[left, piece(i)], right_in.at[i], l_send.at[i], l_recv.at[i], place(d, e, left)))

    for i in order:
        to_left(i) if i < half else to_right(i)
    quarter(t)

    for i in order:
        remote(fwd_in.at[i], fwd_in.at[i], f_send.at[i], f_recv.at[i], place(d, e, right)).wait_recv()
        on = right if i < half else left
        parts[on, piece(i)] = (parts[on, piece(i)].astype(F32) + fwd_in[i].astype(F32)).astype(BF16)
        to_right(i) if i < half else to_left(i)

    for i in order:
        remote(left_in.at[i], left_in.at[i], r_send.at[i], r_recv.at[i], place(d, e, right)).wait_recv()
        remote(right_in.at[i], right_in.at[i], l_send.at[i], l_recv.at[i], place(d, e, left)).wait_recv()
        total = parts[t, piece(i)].astype(F32) + left_in[i].astype(F32) + right_in[i].astype(F32)
        reduced[i] = total.astype(BF16)
        if i > 0:
            go(remote(reduced.at[i], copy_in.at[i], c_send.at[i], c_recv.at[i],
                      place(d, holder(piece(i)), t)))
    total = reduced[0].astype(F32)
    for i in range(1, copies):
        remote(copy_in.at[i], copy_in.at[i], c_send.at[i], c_recv.at[i], place(d, e, right)).wait_recv()
        total = total + copy_in[i].astype(F32)
    finished[...] = total.astype(BF16)

    to_everyone(lambda to: remote(
        finished.at[to], back.at[k, p], back_sem.at[0], back_sem.at[1], place(d, to, t)).start())

    back[k, p] = finished[e]
    bulk = arrived.at[0, pl.ds(0, n_e - 1)]
    back_bulk = remote(bulk, bulk, back_sem.at[0], back_sem.at[1], place(d, e, right))
    back_bulk.wait_recv()

    ys, gs = [], []
    for c in range(copies):
        first, second = split_rows(back[:, c].astype(F32))
        ys.append(first.astype(BF16))
        gs.append(second.astype(BF16))
    y, g = jnp.concatenate(ys, axis=1), jnp.concatenate(gs, axis=1)
    chosen0 = jnp.dot(sel0, y, preferred_element_type=F32)
    chosen1 = jnp.dot(sel1, y, preferred_element_type=F32)
    grad_mix = jnp.dot(sel0 + sel1, g, preferred_element_type=F32)
    rows = toks.shape[0]
    diff = jnp.sum(cots * (chosen0 - chosen1), axis=1, keepdims=True)
    dots = jnp.sum(grad_mix * gains * toks, axis=1, keepdims=True)
    column = lax.broadcasted_iota(jnp.int32, (rows, LANES), 1)
    scal_out[...] = jnp.where(column == 0, diff, jnp.where(column == 1, dots, 0.0))
    mixed_all[t] = (toks + (p0 * chosen0 + p1 * chosen1)).astype(BF16)
    for o in range(1, n_t):
        go(remote(scal_out, scal_in.at[o - 1], sc_send.at[o - 1], sc_recv.at[o - 1], place(d, e, (t + o) % n_t)))
    for o in range(1, n_t):
        go(remote(mixed_all.at[t], mixed_all.at[t], mx_send.at[o - 1], mx_recv.at[o - 1],
                  place(d, e, (t + o) % n_t)))
    scalars = scal_out[...]
    for o in range(1, n_t):
        remote(scal_in.at[o - 1], scal_in.at[o - 1], sc_send.at[o - 1], sc_recv.at[o - 1],
               place(d, e, right)).wait_recv()
        scalars = scalars + scal_in[o - 1]
    grad_first = p0 * p1 * scalars[:, 0:1]
    grad_logits = grad_first * sign
    grad_normed = grad_mix
    routers = router_ref[:, sl].astype(F32)
    for j in range(experts):
        grad_normed = grad_normed + grad_logits[:, j : j + 1] * routers[j : j + 1]
    normed32 = normeds.astype(F32)
    router_part = jnp.concatenate(
        [jnp.sum(grad_logits[:, j : j + 1] * normed32, axis=0, keepdims=True) for j in range(experts)], axis=0)
    gain_part = jnp.sum(grad_normed * toks * inv_rms, axis=0, keepdims=True)
    units = sums.shape[1]

    def unit(u):
        return u // units, u % units

    n_half = experts // SLOTS
    for c in range(copies):
        at = slice(c * LANES, (c + 1) * LANES)
        for h in range(n_half):
            a, b = unit(c * n_half + h)
            sums[a, b] = router_part[h * SLOTS : (h + 1) * SLOTS, at]
        a, b = unit(n_half * copies + c // SLOTS)
        sums[a, b, c % SLOTS : c % SLOTS + 1] = gain_part[:, at]

    near = far_first(LINE) + [0]
    members = []
    for dy in near:
        for dd in range(n_dp):
            if dy or dd:
                there = modulo(d + dd, n_dp)
                members.append((there * LINE + rows_of[dy], place(there, z * LINE + rows_of[dy], t)))

    for j, target in members:
        remote(sums.at[j], line_in.at[line], line_sem.at[0], line_sem.at[1], target).start()

    mean = (scalars[:, 1:2] + jnp.sum(grad_logits * through, axis=1, keepdims=True)) / (n_t * width)
    cubed = inv_rms * inv_rms * inv_rms
    gtok_all[t] = (cots + inv_rms * (grad_normed * gains) - toks * cubed * mean).astype(BF16)
    for o in range(1, n_t):
        go(remote(gtok_all.at[t], gtok_all.at[t], gt_send.at[o - 1], gt_recv.at[o - 1],
                  place(d, e, (t + o) % n_t)))
    line_in[line] = sums[line]
    some = pl.ds(0, n_line - 1)
    line_bulk = remote(line_in.at[some], line_in.at[some], line_sem.at[0], line_sem.at[1], place(d, e, right))
    line_bulk.wait_recv()
    line_sum[...] = jnp.sum(line_in[...], axis=0)

    if n_z > 1:
        for dz in far_first(n_z):
            remote(line_sum, z_in.at[z], z_sem.at[0], z_sem.at[1], place(d, plane_of[dz] + rows_of[0], t)).start()

        z_in[z] = line_sum[...]
        zs = pl.ds(0, n_z - 1)
        z_bulk = remote(z_in.at[zs], z_in.at[zs], z_sem.at[0], z_sem.at[1], place(d, e, right))
        z_bulk.wait_recv()
        z_sum[...] = jnp.sum(z_in[...], axis=0)
    else:
        z_sum[...] = line_sum[...]

    for j, target in members:
        remote(z_sum, grads.at[t, line], gl_sem.at[0], gl_sem.at[1], target).start()

    grads[t, line] = z_sum[...]
    gl_bulk = remote(grads.at[t, some], grads.at[t, some], gl_sem.at[0], gl_sem.at[1], place(d, e, right))
    gl_bulk.wait_recv()
    for o in range(1, n_t):
        go(remote(grads.at[t], grads.at[t], gx_send.at[o - 1], gx_recv.at[o - 1], place(d, e, (t + o) % n_t)))

    def other(o):
        return (t + n_t - o) % n_t

    for o in range(1, n_t):
        remote(mixed_all.at[other(o)], mixed_all.at[other(o)], mx_send.at[o - 1], mx_recv.at[o - 1],
               place(d, e, right)).wait_recv()
        remote(gtok_all.at[other(o)], gtok_all.at[other(o)], gt_send.at[o - 1], gt_recv.at[o - 1],
               place(d, e, right)).wait_recv()
    for o in range(1, n_t):
        remote(grads.at[other(o)], grads.at[other(o)], gx_send.at[o - 1], gx_recv.at[o - 1],
               place(d, e, right)).wait_recv()

    a2a.wait_send()
    back_bulk.wait_send()
    line_bulk.wait_send()
    if n_z > 1:
        z_bulk.wait_send()
    gl_bulk.wait_send()
    for copy in started:
        copy.wait_send()


def assemble_kernel(dims, mixed_all, gtok_all, grads, mixed_ref, gtok_ref, grouter_ref, ggain_ref):
    n_dp, n_e, n_t, experts, copies = dims
    width, n_half, units = copies * LANES, experts // SLOTS, grads.shape[2]

    def unit(u):
        return u // units, u % units

    for q in range(n_t):
        at = slice(q * width, (q + 1) * width)
        mixed_ref[:, at] = mixed_all[q]
        gtok_ref[:, at] = gtok_all[q]
        for c in range(copies):
            at = slice(q * width + c * LANES, q * width + (c + 1) * LANES)
            for h in range(n_half):
                a, b = unit(c * n_half + h)
                grouter_ref[h * SLOTS : (h + 1) * SLOTS, at] = grads[q, a, b]
            a, b = unit(n_half * copies + c // SLOTS)
            ggain_ref[:, at] = grads[q, a, b, c % SLOTS : c % SLOTS + 1]


def shards(dims, tokens, cotangent, gain, w_router, w_gate, w_up, w_down, expert_ids, slots):
    n_dp, n_e, n_t, experts, copies = dims
    count, features = tokens.shape
    hidden = w_gate.shape[2]
    width = features // n_t
    n_rows = n_e * SLOTS
    n_line, n_z = n_dp * LINE, n_e // LINE
    units = -(-(copies * (experts // SLOTS) + -(-copies // SLOTS)) // n_line)
    block = (n_e, 8, LANES)
    dma = pltpu.SemaphoreType.DMA
    vmem = pl.BlockSpec(memory_space=pltpu.VMEM)
    scratch = [
        pltpu.VMEM((n_t, width, hidden), BF16), pltpu.VMEM((n_t, width, hidden), BF16),
        pltpu.VMEM((hidden, features), BF16),
        pltpu.VMEM((experts, copies, 8, LANES), BF16),
        pltpu.VMEM((n_t * copies,) + block, BF16),
        pltpu.VMEM((n_rows, width), BF16), pltpu.VMEM((n_rows, width), BF16),
        pltpu.VMEM((3, n_rows, hidden), F32), pltpu.VMEM((3, n_rows, hidden), BF16),
        pltpu.VMEM((n_t, copies) + block, BF16),
        pltpu.VMEM((copies,) + block, BF16), pltpu.VMEM((copies,) + block, BF16),
        pltpu.VMEM((copies,) + block, BF16), pltpu.VMEM((copies,) + block, BF16),
        pltpu.VMEM((copies,) + block, BF16),
        pltpu.VMEM(block, BF16),
        pltpu.VMEM((experts, copies, 8, LANES), BF16),
        pltpu.VMEM((count, LANES), F32), pltpu.VMEM((n_t - 1, count, LANES), F32),
        pltpu.VMEM((n_line, units, SLOTS, LANES), F32), pltpu.VMEM((n_line, units, SLOTS, LANES), F32),
        pltpu.VMEM((units, SLOTS, LANES), F32),
        pltpu.VMEM((n_z, units, SLOTS, LANES), F32), pltpu.VMEM((units, SLOTS, LANES), F32),
        dma((3,)), dma((2,)),
    ] + [dma((copies, BANDS))] * 8 + [dma((copies,))] * 8 + [dma((2,))] + [dma((n_t - 1,))] * 6 + [dma((2,))] * 3 + [dma((n_t - 1,))] * 2
    gathered = pl.pallas_call(
        functools.partial(layer_kernel, dims),
        out_shape=(
            jax.ShapeDtypeStruct((n_t, count, width), BF16), jax.ShapeDtypeStruct((n_t, count, width), BF16),
            jax.ShapeDtypeStruct((n_t, n_line, units, SLOTS, LANES), F32),
        ),
        in_specs=[vmem] * 6 + [pl.BlockSpec(memory_space=pl.ANY)] * 3,
        out_specs=(vmem,) * 3,
        scratch_shapes=scratch,
        compiler_params=pltpu.CompilerParams(
            collective_id=0, has_side_effects=True, vmem_limit_bytes=56 * 1024 * 1024),
    )(
        tokens, cotangent, gain.reshape(1, features), w_router.T, expert_ids.T, slots.T,
        w_gate.reshape(n_t, width, hidden), w_up.reshape(n_t, width, hidden), w_down.reshape(hidden, features),
    )
    mixed, gtok, grouter, ggain = pl.pallas_call(
        functools.partial(assemble_kernel, dims),
        out_shape=(
            jax.ShapeDtypeStruct((count, features), BF16), jax.ShapeDtypeStruct((count, features), BF16),
            jax.ShapeDtypeStruct((experts, features), F32), jax.ShapeDtypeStruct((1, features), F32),
        ),
        in_specs=[vmem] * 3,
        out_specs=(vmem,) * 4,
    )(*gathered)
    return mixed, gtok, grouter.T, ggain.reshape(features)


def solution(mesh):
    n_dp, n_e, n_t = (mesh.shape[a] for a in ("dp", "expert", "tensor"))

    def body(*args):
        experts = args[3].shape[1]
        return shards((n_dp, n_e, n_t, experts, n_e // experts), *args)

    return jax.shard_map(
        body,
        mesh=mesh,
        in_specs=(
            P(("dp", "expert"), None),
            P(("dp", "expert"), None),
            P(),
            P(),
            P("expert", None, "tensor"),
            P("expert", None, "tensor"),
            P("expert", "tensor", None),
            P(("dp", "expert"), None),
            P(("dp", "expert"), None),
        ),
        out_specs=(P(("dp", "expert"), None), P(("dp", "expert"), None), P(), P()),
        check_vma=False,
    )
```
